512 devices in a mesh: grp: 2 (over y), gx: 32 (over z), gy: 4 (over x), gz: 2 (over core).
Axes of the slice: x: 4, y: 2, z: 32, core: 2. Of those that a mesh axis runs over, the one named last changes fastest.
The devices are a block of a 4x8x32 slice.
Arguments:
- position: float32 [64, 128, 8, 256], P(None, ('grp', 'gx'), 'gy', 'gz'), parts along dimension 1, may hold values from -6 to 6
- momentum: float32 [64, 128, 8, 256], P(None, ('grp', 'gx'), 'gy', 'gz'), parts along dimension 1, may hold values from -6 to 6
- noise: bfloat16 [3, 64, 128, 8, 256], P(None, None, ('grp', 'gx'), 'gy', 'gz'), parts along dimension 2, may hold values from -6 to 6
- filter_in: bfloat16 [64, 64, 3, 3, 3], P('gx', 'gy'), may hold values from -0.15625 to 0.15625
- filter_out: bfloat16 [64, 64, 3, 3, 3], P('gx', 'gy'), may hold values from -0.15625 to 0.15625
- bias: float32 [64], replicated, may hold values from -4 to 4
Outputs:
- final_position: float32 [64, 128, 8, 256], P(None, ('grp', 'gx'), 'gy', 'gz'), parts along dimension 1
- final_momentum: float32 [64, 128, 8, 256], P(None, ('grp', 'gx'), 'gy', 'gz'), parts along dimension 1
The draws below stay inside these ranges and needn't reach their ends.
There are 2 independent parts, one for each index of `grp`. The reference program is written for one: setup_inputs(seed, part) draws one part's arguments, and reference() takes and returns one part's arrays. A program takes and returns all parts, laid end to end along the dimension named above; an argument that names none is the same for every part. Nothing has to cross between parts.
All inputs are finite; a program needn't handle non-finite values.
Results may differ from the reference program's by a relative error of at most 0.0013.
Values may be sent and summed in bfloat16 or wider, within the bound.
No kernel may reach another device: no remote copies, remote signals or barrier semaphores. Data moves between devices by JAX's collectives and lax.ppermute only.
A program may use at most 64 MiB of HBM per device.

```python
import jax
import jax.numpy as jnp
from jax import lax

C = 64
STEPS = 3
NX = 64
NY = 8
NZ = 256


def block_scale(own_key, shape, pieces, smallest, top_value):
    def one(axis_at, parts):
        steps = jax.random.uniform(jax.random.fold_in(jax.random.fold_in(own_key, 6), axis_at), (parts,), jnp.float32, smallest / len(pieces), top_value / len(pieces))
        return jnp.repeat(jnp.exp(steps), shape[axis_at] // parts).reshape((-1,) + (1,) * (len(shape) - axis_at - 1))

    loudness = one(*pieces[0])
    for cut in pieces[1:]:
        loudness = loudness * one(*cut)
    return loudness


def scatter_about(key, dims, scale, most, pieces=(), kind=jnp.bfloat16):
    drawn = jax.random.normal(key, dims, jnp.float32) * scale
    if len(pieces) > 0:
        drawn = block_scale(key, dims, pieces, -0.22, 0.18) * drawn
    return jnp.clip(drawn, min=-most, max=most).astype(kind)


def setup_inputs(seed: int = 0, part: int = 0) -> dict:
    streams_of = jax.random.split(jax.random.key(seed), 7)
    part_splits = jax.random.split(jax.random.fold_in(streams_of[6], part), 7)
    position = scatter_about(part_splits[0], (C, NX, NY, NZ), 1.0, 6.0, ((1, 32), (2, 4), (3, 2)), jnp.float32)
    momentum = scatter_about(part_splits[1], (C, NX, NY, NZ), 1.0, 6.0, ((1, 32), (2, 4), (3, 2)), jnp.float32)
    noise = scatter_about(part_splits[2], (STEPS, C, NX, NY, NZ), 1.0, 6.0, ((2, 32), (3, 4), (4, 2)))
    filter_in = scatter_about(streams_of[3], (C, C, 3, 3, 3), (27 * C) ** -0.5, 0.15625, ((0, 32), (1, 4)))
    filter_out = scatter_about(streams_of[4], (C, C, 3, 3, 3), (27 * C) ** -0.5, 0.15625, ((0, 32), (1, 4)))
    bias = scatter_about(streams_of[5], (C,), 1.0, 4.0, (), jnp.float32)
    return {"position": position, "momentum": momentum, "noise": noise, "filter_in": filter_in, "filter_out": filter_out, "bias": bias}


def convolve(field, filters):
    padded = jnp.pad(field, ((0, 0), (1, 1), (1, 1), (1, 1)), mode='wrap')
    return lax.conv_general_dilated(padded[None], filters, (1, 1, 1), 'VALID', dimension_numbers=('NCDHW', 'OIDHW', 'NCDHW'), preferred_element_type=jnp.float32)[0]

def adjoint(filters):
    return jnp.transpose(jnp.flip(filters, (2, 3, 4)), (1, 0, 2, 3, 4))

def reference(position, momentum, noise, filter_in, filter_out, bias):
    back_in = adjoint(filter_in)
    back_out = adjoint(filter_out)
    bias_col = bias[:, None, None, None]

    def gradient(field):
        rounded = field.astype(jnp.bfloat16)
        pre = convolve(rounded, filter_in) + bias_col
        active = jnp.tanh(pre)
        output = convolve(active.astype(jnp.bfloat16), filter_out)
        back = convolve(output.astype(jnp.bfloat16), back_out)
        hidden = (back * (1.0 - active * active)).astype(jnp.bfloat16)
        return convolve(hidden, back_in) + field
    step = 0.25
    decay = jnp.exp(jnp.float32(-0.25))
    kick = jnp.sqrt(1.0 - decay * decay)
    field = position
    moment = momentum
    force = gradient(field)
    for index in range(STEPS):
        moment = moment - 0.5 * step * force
        field = field + 0.5 * step * moment
        moment = decay * moment + kick * noise[index].astype(jnp.float32)
        field = field + 0.5 * step * moment
        force = gradient(field)
        moment = moment - 0.5 * step * force
    return (field, moment)
```

```python
import functools
import math

import jax
import jax.numpy as jnp
from jax import lax
from jax.experimental import pallas as pl
from jax.experimental.pallas import tpu as pltpu
from jax.sharding import Mesh, PartitionSpec as P

F32, BF16 = jnp.float32, jnp.bfloat16
STEP = 0.25
XB, ZB = 4, 16
HALO = 4
PITCH = ZB + 2 * HALO
VMEM = pltpu.VMEM
LIMIT = 24 * 1024 * 1024


def cycle(rows, cols):
    path = [(0, b) for b in range(cols)]
    for b in range(cols - 1, 0, -1):
        column = [(a, b) for a in range(1, rows)]
        path += column if (cols - 1 - b) % 2 == 0 else column[::-1]
    return path + [(a, 0) for a in range(rows - 1, 0, -1)]


def kernel_call(body, outs, args, scratch=(), name=None):
    spec = pl.BlockSpec(memory_space=VMEM)
    args = [pltpu.with_memory_space_constraint(v, VMEM) for v in args]
    return pl.pallas_call(
        body,
        out_shape=[VMEM(o.shape, o.dtype) for o in outs],
        in_specs=[spec] * len(args),
        out_specs=[spec] * len(outs),
        scratch_shapes=list(scratch),
        compiler_params=pltpu.CompilerParams(vmem_limit_bytes=LIMIT),
        name=name,
    )(*args)


def spread_body(place, q_ref, p_ref, n_ref, out_ref):
    for k in range(2 + n_ref.shape[0]):
        for x in range(q_ref.shape[1]):
            if k < 2:
                ref = (q_ref, p_ref)[k]
                parts = [ref[:, x, y, :] for y in range(ref.shape[2])]
            else:
                parts = [n_ref[k - 2, :, x, y, :].astype(F32) for y in range(n_ref.shape[3])]
            flat = jnp.concatenate(parts, axis=0).T
            for member, block in enumerate(place):
                out_ref[member, k, x] = flat[block * ZB : (block + 1) * ZB, :]


def collect_body(place, in_ref, q_ref, p_ref):
    for k, ref in enumerate((q_ref, p_ref)):
        chans = ref.shape[0]
        for x in range(ref.shape[1]):
            rows = [None] * len(place)
            for member, block in enumerate(place):
                rows[block] = in_ref[member, k, x]
            flat = jnp.concatenate(rows, axis=0).T
            for y in range(ref.shape[2]):
                ref[:, x, y, :] = flat[y * chans : (y + 1) * chans, :]


def weights_body(m_ref, out_ref, fwd_ref):
    groups, chans, _ = m_ref.shape
    per = chans // groups
    taps = 27
    turned = [m_ref[g].astype(F32).T.astype(BF16) for g in range(groups)]
    for f in range(2):
        for tap in range(taps):
            at = (f * taps + tap) * per
            for g in range(groups):
                fwd_ref[f, tap * chans + g * per : tap * chans + (g + 1) * per, :] = turned[g][
                    at : at + per, :
                ].astype(F32)
    zero = jnp.zeros((chans, chans), BF16)

    def place(w, tap, block):
        a, b, c = tap // 9, tap // 3 % 3, tap % 3
        for u in range(2):
            t = b + u
            row = ((t // 2 * 3 + c) * 2 + t % 2) * chans
            col = (a * 2 + u) * chans
            out_ref[w, row : row + chans, col : col + chans] = block

    for w in range(4):
        for c in range(3):
            for a in range(3):
                for t, u in ((3, 0), (0, 1)):
                    row = ((t // 2 * 3 + c) * 2 + t % 2) * chans
                    col = (a * 2 + u) * chans
                    out_ref[w, row : row + chans, col : col + chans] = zero
    for f in range(2):
        for tap in range(0, taps, 2):
            n = min(2, taps - tap)
            pair = fwd_ref[f, tap * chans : (tap + n) * chans, :]
            adj = pair.T
            for i in range(n):
                part = slice(i * chans, (i + 1) * chans)
                place(f, tap + i, pair[part].astype(BF16))
                place(f + 2, taps - 1 - tap - i, adj[:, part].astype(BF16))


def gradient_body(kind, coef, *refs):
    decay, kick = coef
    it = iter(refs)
    r_ref = next(it)
    if kind == "first":
        q_of = lambda x, j: r_ref[x // 2 * 4 + j, 0, x % 2]
        p_of = lambda x, j: r_ref[x // 2 * 4 + j, 1, x % 2]
    else:
        q_ref, p_ref = next(it), next(it)
        q_of = lambda x, j: q_ref[x, j]
        p_of = lambda x, j: p_ref[x, j]
    xl_ref, xh_ref, zl_ref, zh_ref, w_ref, bias_ref = (next(it) for _ in range(6))
    if kind == "last":
        out_ref = next(it)
    else:
        qo_ref, po_ref, qb_ref = (next(it) for _ in range(3))
    buf, rows_ref, act = (next(it) for _ in range(3))
    step_at = {"first": 0}.get(kind, kind)

    x_all = XB + 2 * HALO
    lo, hi = 8 + HALO, 8 + HALO + ZB
    edge = jnp.zeros((x_all, 4, 8, 128), F32)
    buf[:, :, 0:8, :] = edge
    buf[:, :, 8 + PITCH : 16 + PITCH, :] = edge
    buf[0:HALO, :, lo:hi, :] = xl_ref[...].astype(F32)
    buf[HALO + XB :, :, lo:hi, :] = xh_ref[...].astype(F32)
    for x in range(XB):
        for j in range(4):
            buf[HALO + x, j, lo:hi, :] = q_of(x, j)
    buf[:, :, 8:lo, :] = zl_ref[...].astype(F32)
    buf[:, :, hi : 8 + PITCH, :] = zh_ref[...].astype(F32)

    def conv(x_in, w, use):
        n = x_in * PITCH
        for j in range(4):
            for c in range(3):
                v = buf[0:x_in, j, 7 + c : 7 + c + PITCH, :].reshape(n, 128).astype(BF16)
                rows_ref[0:n, (j * 3 + c) * 128 : (j * 3 + c + 1) * 128] = v
                if j == 0:
                    rows_ref[0:n, (12 + c) * 128 : (13 + c) * 128] = v
        x_out = x_in - 2
        m = x_out * PITCH
        for p in range(4):
            t = jnp.dot(
                rows_ref[0:n, 384 * p : 384 * p + 768], w_ref[w], preferred_element_type=F32
            )
            o = t[0:m, 0:128] + t[PITCH : PITCH + m, 128:256] + t[2 * PITCH :, 256:384]
            use(p, o.reshape(x_out, PITCH, 128))

    def hidden(p, h):
        t = jnp.tanh(h + bias_ref[...])
        act[:, p] = 1.0 - t * t
        buf[0 : XB + 6, p, 8 : 8 + PITCH, :] = t

    def second(p, h):
        buf[0 : XB + 4, p, 8 : 8 + PITCH, :] = h

    def back(p, g):
        buf[0 : XB + 2, p, 8 : 8 + PITCH, :] = g * act[2 : XB + 4, (p + 1) % 4]

    half = 0.5 * STEP

    def final(p, g):
        buf[0:XB, p, 8 : 8 + PITCH, :] = g
        j = (p + 2) % 4
        for x in range(XB):
            q = q_of(x, j)
            force = buf[x, p, lo:hi, :] + q
            mom = p_of(x, j) - half * force
            if kind == "last":
                out_ref[x // 2, j, 0, x % 2] = q
                out_ref[x // 2, j, 1, x % 2] = mom
                continue
            if kind != "first":
                mom = mom - half * force
            q = q + half * mom
            mom = decay * mom + kick * r_ref[x // 2 * 4 + j, 2 + step_at, x % 2]
            q = q + half * mom
            qo_ref[x, j] = q
            po_ref[x, j] = mom
            qb_ref[x, j] = q.astype(BF16)

    conv(XB + 8, 0, hidden)
    conv(XB + 6, 1, second)
    conv(XB + 4, 3, back)
    conv(XB + 2, 2, final)


def solution(mesh):
    gy, gz = mesh.shape["gy"], mesh.shape["gz"]
    gs = XB // 2
    gX = mesh.shape["gx"] // gs
    fine = Mesh(
        mesh.devices.reshape(mesh.shape["grp"], gX, gs, gy, gz), ("grp", "gX", "gs", "gy", "gz")
    )
    walk = cycle(gs, gy)
    place = [walk.index((a, b)) for a in range(gs) for b in range(gy)]
    ring = [(a * gy + b) * gz + c for c in range(gz) for a, b in walk]

    def x_shift(d):
        return [(i, (i + d) % gX) for i in range(gX)]

    def z_shift(d):
        n = len(ring)
        return [(ring[i], ring[(i + d) % n]) for i in range(n)]

    decay = math.exp(-0.25)
    kick = math.sqrt(1.0 - decay * decay)

    def halos(block):
        xl = lax.ppermute(block, "gX", x_shift(1))
        xh = lax.ppermute(block, "gX", x_shift(-1))
        whole = jnp.concatenate([xl, block, xh], axis=0)
        zl = lax.ppermute(whole[:, :, ZB - HALO :], ("gs", "gy", "gz"), z_shift(1))
        zh = lax.ppermute(whole[:, :, :HALO], ("gs", "gy", "gz"), z_shift(-1))
        return xl, xh, zl, zh

    def on_device(position, momentum, noise, filter_in, filter_out, bias):
        chans = position.shape[0]
        steps = noise.shape[0]
        members = gs * gy

        own = [f.reshape(*f.shape[:2], 27).transpose(0, 2, 1) for f in (filter_in, filter_out)]
        own = jnp.concatenate([f.reshape(f.shape[0], -1) for f in own], axis=1)
        own = jnp.pad(own, ((0, 0), (0, -own.shape[1] % 128)))
        far = lax.all_to_all(
            jnp.broadcast_to(own, (gX, *own.shape)), "gX", 0, 0, tiled=True
        )
        far = far.reshape(-1, far.shape[-1])
        near = lax.all_to_all(
            jnp.broadcast_to(far, (members, *far.shape)), ("gs", "gy"), 0, 0, tiled=True
        )
        near = near.reshape(gs, gy, gX, *own.shape).transpose(1, 2, 0, 3, 4)
        (weights,) = kernel_call(
            weights_body,
            [jax.ShapeDtypeStruct((4, 12 * chans, 6 * chans), BF16)],
            (near.reshape(gy, chans, own.shape[1]),),
            [VMEM((2, 27 * chans, chans), F32)],
            name="weights",
        )
        bias_row = jnp.concatenate([bias, bias])[None, :]

        (spread,) = kernel_call(
            functools.partial(spread_body, place),
            [jax.ShapeDtypeStruct((members, 2 + steps, 2, ZB, 128), F32)],
            (position, momentum, noise),
            name="spread",
        )
        held = lax.all_to_all(spread, ("gs", "gy"), 0, 0, tiled=True)

        start = held[:, 0].reshape(gs, gy, 2, ZB, 128).transpose(0, 2, 1, 3, 4)
        block = start.reshape(XB, gy, ZB, 128).astype(BF16)

        shape = jax.ShapeDtypeStruct(block.shape, F32)
        scratch = (
            VMEM((XB + 8, gy, PITCH + 16, 128), F32),
            VMEM(((XB + 8) * PITCH, 15 * 128), BF16),
            VMEM((XB + 6, gy, PITCH, 128), F32),
        )
        coef = (decay, kick)
        state = ()
        for k in range(steps + 1):
            kind = "first" if k == 0 else "last" if k == steps else k
            edges = halos(block)
            args = (held, *state, *edges, weights, bias_row)
            if kind == "last":
                outs = [jax.ShapeDtypeStruct((gs, gy, 2, 2, ZB, 128), F32)]
            else:
                outs = [shape, shape, jax.ShapeDtypeStruct(block.shape, BF16)]
            res = kernel_call(
                functools.partial(gradient_body, kind, coef), outs, args, scratch, name="gradient"
            )
            if kind != "last":
                state, block = tuple(res[:2]), res[2]
        back = lax.all_to_all(
            res[0].reshape(members, 2, 2, ZB, 128), ("gs", "gy"), 0, 0, tiled=True
        )
        out = jax.ShapeDtypeStruct(position.shape, F32)
        return tuple(
            kernel_call(functools.partial(collect_body, place), [out, out], (back,), name="collect")
        )

    where = ("grp", "gX", "gs")
    lattice = P(None, where, "gy", "gz")
    filters = P(("gX", "gs"), "gy", None, None, None)
    return jax.shard_map(
        on_device,
        mesh=fine,
        in_specs=(lattice, lattice, P(None, None, where, "gy", "gz"), filters, filters, P()),
        out_specs=(lattice, lattice),
        check_vma=False,
    )
```

```python
import functools
import math

import jax
import jax.numpy as jnp
from jax import lax
from jax.experimental import pallas as pl
from jax.experimental.pallas import tpu as pltpu
from jax.sharding import Mesh, PartitionSpec as P


F32, BF16 = jnp.float32, jnp.bfloat16
STEP = 0.25
XB, ZB = 4, 16
HALO = 4
PITCH = ZB + 2 * HALO
VMEM = pltpu.VMEM
LIMIT = 24 * 1024 * 1024


def cycle(rows, cols):
    path = [(0, b) for b in range(cols)]
    for b in range(cols - 1, 0, -1):
        column = [(a, b) for a in range(1, rows)]
        path += column if (cols - 1 - b) % 2 == 0 else column[::-1]
    return path + [(a, 0) for a in range(rows - 1, 0, -1)]


def kernel_call(body, outs, args, scratch=(), hbm_in=False, hbm_out=False):
    spec = pl.BlockSpec(memory_space=VMEM)
    space = pltpu.HBM if hbm_in else VMEM
    args = [pltpu.with_memory_space_constraint(v, space) for v in args]
    return pl.pallas_call(
        body,
        out_shape=outs if hbm_out else [VMEM(o.shape, o.dtype) for o in outs],
        in_specs=[spec] * len(args),
        out_specs=[spec] * len(outs),
        scratch_shapes=list(scratch),
        compiler_params=pltpu.CompilerParams(vmem_limit_bytes=LIMIT),
    )(*args)


def spread_body(place, q_ref, p_ref, n_ref, out_ref):
    for k in range(2 + n_ref.shape[0]):
        for x in range(q_ref.shape[1]):
            if k < 2:
                ref = (q_ref, p_ref)[k]
                parts = [ref[:, x, y, :] for y in range(ref.shape[2])]
            else:
                parts = [n_ref[k - 2, :, x, y, :].astype(F32) for y in range(n_ref.shape[3])]
            flat = jnp.concatenate(parts, axis=0).T
            for member, block in enumerate(place):
                out_ref[member, k, x] = flat[block * ZB : (block + 1) * ZB, :]


def collect_body(place, in_ref, q_ref, p_ref):
    for k, ref in enumerate((q_ref, p_ref)):
        chans = ref.shape[0]
        for x in range(ref.shape[1]):
            rows = [None] * len(place)
            for member, block in enumerate(place):
                rows[block] = in_ref[member, k, x]
            flat = jnp.concatenate(rows, axis=0).T
            for y in range(ref.shape[2]):
                ref[:, x, y, :] = flat[y * chans : (y + 1) * chans, :]


def weights_body(m_ref, out_ref, fwd_ref):
    groups, chans, _ = m_ref.shape
    per = chans // groups
    taps = 27
    turned = [m_ref[g].astype(F32).T.astype(BF16) for g in range(groups)]
    for f in range(2):
        for tap in range(taps):
            at = (f * taps + tap) * per
            for g in range(groups):
                fwd_ref[f, tap * chans + g * per : tap * chans + (g + 1) * per, :] = turned[g][
                    at : at + per, :
                ].astype(F32)
    zero = jnp.zeros((chans, chans), BF16)

    def place(w, tap, block):
        a, b, c = tap // 9, tap // 3 % 3, tap % 3
        for u in range(2):
            t = b + u
            row = ((t // 2 * 3 + c) * 2 + t % 2) * chans
            col = (a * 2 + u) * chans
            out_ref[w, row : row + chans, col : col + chans] = block

    for w in range(4):
        for c in range(3):
            for a in range(3):
                for t, u in ((3, 0), (0, 1)):
                    row = ((t // 2 * 3 + c) * 2 + t % 2) * chans
                    col = (a * 2 + u) * chans
                    out_ref[w, row : row + chans, col : col + chans] = zero
    for f in range(2):
        for tap in range(0, taps, 2):
            n = min(2, taps - tap)
            pair = fwd_ref[f, tap * chans : (tap + n) * chans, :]
            adj = pair.T
            for i in range(n):
                part = slice(i * chans, (i + 1) * chans)
                place(f, tap + i, pair[part].astype(BF16))
                place(f + 2, taps - 1 - tap - i, adj[:, part].astype(BF16))


def gradient_body(kind, coef, *refs):
    decay, kick = coef
    it = iter(refs)
    r_ref = next(it)
    if kind == "first":
        q_of = lambda x, j: r_ref[x // 2 * 4 + j, 0, x % 2]
        p_of = lambda x, j: r_ref[x // 2 * 4 + j, 1, x % 2]
    else:
        q_ref, p_ref = next(it), next(it)
        q_of = lambda x, j: q_ref[x, j]
        p_of = lambda x, j: p_ref[x, j]
    xl_ref, xh_ref, zl_ref, zh_ref, w_ref, bias_ref = (next(it) for _ in range(6))
    if kind == "last":
        out_ref = next(it)
    else:
        qo_ref, po_ref, qb_ref = (next(it) for _ in range(3))
    buf, rows_ref, act = (next(it) for _ in range(3))
    step_at = {"first": 0}.get(kind, kind)

    x_all = XB + 2 * HALO
    lo, hi = 8 + HALO, 8 + HALO + ZB
    edge = jnp.zeros((x_all, 4, 8, 128), F32)
    buf[:, :, 0:8, :] = edge
    buf[:, :, 8 + PITCH : 16 + PITCH, :] = edge
    buf[0:HALO, :, lo:hi, :] = xl_ref[...].astype(F32)
    buf[HALO + XB :, :, lo:hi, :] = xh_ref[...].astype(F32)
    for x in range(XB):
        for j in range(4):
            buf[HALO + x, j, lo:hi, :] = q_of(x, j)
    buf[:, :, 8:lo, :] = zl_ref[...].astype(F32)
    buf[:, :, hi : 8 + PITCH, :] = zh_ref[...].astype(F32)

    def conv(x_in, w, use):
        n = x_in * PITCH
        for j in range(4):
            for c in range(3):
                v = buf[0:x_in, j, 7 + c : 7 + c + PITCH, :].reshape(n, 128).astype(BF16)
                rows_ref[0:n, (j * 3 + c) * 128 : (j * 3 + c + 1) * 128] = v
                if j == 0:
                    rows_ref[0:n, (12 + c) * 128 : (13 + c) * 128] = v
        x_out = x_in - 2
        m = x_out * PITCH
        for p in range(4):
            t = jnp.dot(
                rows_ref[0:n, 384 * p : 384 * p + 768], w_ref[w], preferred_element_type=F32
            )
            o = t[0:m, 0:128] + t[PITCH : PITCH + m, 128:256] + t[2 * PITCH :, 256:384]
            use(p, o.reshape(x_out, PITCH, 128))

    def hidden(p, h):
        t = jnp.tanh(h + bias_ref[...])
        act[:, p] = 1.0 - t * t
        buf[0 : XB + 6, p, 8 : 8 + PITCH, :] = t

    def second(p, h):
        buf[0 : XB + 4, p, 8 : 8 + PITCH, :] = h

    def back(p, g):
        buf[0 : XB + 2, p, 8 : 8 + PITCH, :] = g * act[2 : XB + 4, (p + 1) % 4]

    half = 0.5 * STEP

    def final(p, g):
        buf[0:XB, p, 8 : 8 + PITCH, :] = g
        j = (p + 2) % 4
        for x in range(XB):
            q = q_of(x, j)
            force = buf[x, p, lo:hi, :] + q
            mom = p_of(x, j) - half * force
            if kind == "last":
                out_ref[x // 2, j, 0, x % 2] = q
                out_ref[x // 2, j, 1, x % 2] = mom
                continue
            if kind != "first":
                mom = mom - half * force
            q = q + half * mom
            mom = decay * mom + kick * r_ref[x // 2 * 4 + j, 2 + step_at, x % 2]
            q = q + half * mom
            qo_ref[x, j] = q
            po_ref[x, j] = mom
            qb_ref[x, j] = q.astype(BF16)

    conv(XB + 8, 0, hidden)
    conv(XB + 6, 1, second)
    conv(XB + 4, 3, back)
    conv(XB + 2, 2, final)


def solution(mesh):
    gy, gz = mesh.shape["gy"], mesh.shape["gz"]
    gs = XB // 2
    gX = mesh.shape["gx"] // gs
    fine = Mesh(
        mesh.devices.reshape(mesh.shape["grp"], gX, gs, gy, gz), ("grp", "gX", "gs", "gy", "gz")
    )
    walk = cycle(gs, gy)
    place = [walk.index((a, b)) for a in range(gs) for b in range(gy)]
    ring = [(a * gy + b) * gz + c for c in range(gz) for a, b in walk]

    def x_shift(d):
        return [(i, (i + d) % gX) for i in range(gX)]

    def z_shift(d):
        n = len(ring)
        return [(ring[i], ring[(i + d) % n]) for i in range(n)]

    decay = math.exp(-0.25)
    kick = math.sqrt(1.0 - decay * decay)

    def halos(block):
        xl = lax.ppermute(block, "gX", x_shift(1))
        xh = lax.ppermute(block, "gX", x_shift(-1))
        whole = jnp.concatenate([xl, block, xh], axis=0)
        zl = lax.ppermute(whole[:, :, ZB - HALO :], ("gs", "gy", "gz"), z_shift(1))
        zh = lax.ppermute(whole[:, :, :HALO], ("gs", "gy", "gz"), z_shift(-1))
        return xl, xh, zl, zh

    def body(position, momentum, noise, filter_in, filter_out, bias):
        chans = position.shape[0]
        steps = noise.shape[0]
        members = gs * gy

        own = [f.reshape(*f.shape[:2], 27).transpose(0, 2, 1) for f in (filter_in, filter_out)]
        own = jnp.concatenate([f.reshape(f.shape[0], -1) for f in own], axis=1)
        own = jnp.pad(own, ((0, 0), (0, -own.shape[1] % 128)))
        far = lax.all_to_all(
            jnp.broadcast_to(own, (gX, *own.shape)), "gX", 0, 0, tiled=True
        )
        far = far.reshape(-1, far.shape[-1])
        near = lax.all_to_all(
            jnp.broadcast_to(far, (members, *far.shape)), ("gs", "gy"), 0, 0, tiled=True
        )
        near = near.reshape(gs, gy, gX, *own.shape).transpose(1, 2, 0, 3, 4)
        (weights,) = kernel_call(
            weights_body,
            [jax.ShapeDtypeStruct((4, 12 * chans, 6 * chans), BF16)],
            (near.reshape(gy, chans, own.shape[1]),),
            [VMEM((2, 27 * chans, chans), F32)],
        )
        bias_row = jnp.concatenate([bias, bias])[None, :]

        (spread,) = kernel_call(
            functools.partial(spread_body, place),
            [jax.ShapeDtypeStruct((members, 2 + steps, 2, ZB, 128), F32)],
            (position, momentum, noise),
            hbm_in=True,
            hbm_out=True,
        )
        held = lax.all_to_all(spread, ("gs", "gy"), 0, 0, tiled=True)

        start = held[:, 0].reshape(gs, gy, 2, ZB, 128).transpose(0, 2, 1, 3, 4)
        block = start.reshape(XB, gy, ZB, 128).astype(BF16)

        shape = jax.ShapeDtypeStruct(block.shape, F32)
        scratch = (
            VMEM((XB + 8, gy, PITCH + 16, 128), F32),
            VMEM(((XB + 8) * PITCH, 15 * 128), BF16),
            VMEM((XB + 6, gy, PITCH, 128), F32),
        )
        coef = (decay, kick)
        state = ()
        for k in range(steps + 1):
            kind = "first" if k == 0 else "last" if k == steps else k
            edges = halos(block)
            args = (held, *state, *edges, weights, bias_row)
            if kind == "last":
                outs = [jax.ShapeDtypeStruct((gs, gy, 2, 2, ZB, 128), F32)]
            else:
                outs = [shape, shape, jax.ShapeDtypeStruct(block.shape, BF16)]
            res = kernel_call(functools.partial(gradient_body, kind, coef), outs, args, scratch)
            if kind != "last":
                state, block = tuple(res[:2]), res[2]
        back = lax.all_to_all(
            res[0].reshape(members, 2, 2, ZB, 128), ("gs", "gy"), 0, 0, tiled=True
        )
        out = jax.ShapeDtypeStruct(position.shape, F32)
        return tuple(
            kernel_call(functools.partial(collect_body, place), [out, out], (back,), hbm_out=True)
        )

    where = ("grp", "gX", "gs")
    lattice = P(None, where, "gy", "gz")
    filters = P(("gX", "gs"), "gy", None, None, None)
    return jax.shard_map(
        body,
        mesh=fine,
        in_specs=(lattice, lattice, P(None, None, where, "gy", "gz"), filters, filters, P()),
        out_specs=(lattice, lattice),
        check_vma=False,
    )
```

```python
import functools
import math

import jax
import jax.numpy as jnp
from jax import lax
from jax.experimental import pallas as pl
from jax.experimental.pallas import tpu as pltpu
from jax.sharding import Mesh, PartitionSpec as P


F32, BF16 = jnp.float32, jnp.bfloat16
STEP = 0.25
XB, ZB = 4, 16
HALO = 4
VMEM = pltpu.VMEM
LIMIT = 24 * 1024 * 1024


def cycle(rows, cols):
    path = [(0, b) for b in range(cols)]
    for b in range(cols - 1, 0, -1):
        column = [(a, b) for a in range(1, rows)]
        path += column if (cols - 1 - b) % 2 == 0 else column[::-1]
    return path + [(a, 0) for a in range(rows - 1, 0, -1)]


def kernel_call(body, outs, args, scratch=(), hbm_in=False, hbm_out=False):
    spec = pl.BlockSpec(memory_space=VMEM)
    space = pltpu.HBM if hbm_in else VMEM
    args = [pltpu.with_memory_space_constraint(v, space) for v in args]
    return pl.pallas_call(
        body,
        out_shape=outs if hbm_out else [VMEM(o.shape, o.dtype) for o in outs],
        in_specs=[spec] * len(args),
        out_specs=[spec] * len(outs),
        scratch_shapes=list(scratch),
        compiler_params=pltpu.CompilerParams(vmem_limit_bytes=LIMIT),
    )(*args)


def spread_body(place, q_ref, p_ref, n_ref, out_ref):
    for k in range(2 + n_ref.shape[0]):
        for x in range(q_ref.shape[1]):
            if k < 2:
                ref = (q_ref, p_ref)[k]
                parts = [ref[:, x, y, :] for y in range(ref.shape[2])]
            else:
                parts = [n_ref[k - 2, :, x, y, :].astype(F32) for y in range(n_ref.shape[3])]
            flat = jnp.concatenate(parts, axis=0).T
            for member, block in enumerate(place):
                out_ref[member, k, x] = flat[block * ZB : (block + 1) * ZB, :]


def collect_body(place, in_ref, q_ref, p_ref):
    for k, ref in enumerate((q_ref, p_ref)):
        chans = ref.shape[0]
        for x in range(ref.shape[1]):
            rows = [None] * len(place)
            for member, block in enumerate(place):
                rows[block] = in_ref[member, k, x]
            flat = jnp.concatenate(rows, axis=0).T
            for y in range(ref.shape[2]):
                ref[:, x, y, :] = flat[y * chans : (y + 1) * chans, :]


def weights_body(m_ref, out_ref, fwd_ref):
    groups, chans, _ = m_ref.shape
    per = chans // groups
    taps = 27
    turned = [m_ref[g].astype(F32).T.astype(BF16) for g in range(groups)]
    for f in range(2):
        for tap in range(taps):
            at = (f * taps + tap) * per
            for g in range(groups):
                fwd_ref[f, tap * chans + g * per : tap * chans + (g + 1) * per, :] = turned[g][
                    at : at + per, :
                ].astype(F32)
    zero = jnp.zeros((chans, chans), BF16)

    def place(w, tap, block):
        a, b, c = tap // 9, tap // 3 % 3, tap % 3
        for u in range(2):
            t = b + u
            row = ((t // 2 * 3 + c) * 2 + t % 2) * chans
            col = (a * 2 + u) * chans
            out_ref[w, row : row + chans, col : col + chans] = block

    for w in range(4):
        for c in range(3):
            for a in range(3):
                for t, u in ((3, 0), (0, 1)):
                    row = ((t // 2 * 3 + c) * 2 + t % 2) * chans
                    col = (a * 2 + u) * chans
                    out_ref[w, row : row + chans, col : col + chans] = zero
    for f in range(2):
        for tap in range(0, taps, 2):
            n = min(2, taps - tap)
            pair = fwd_ref[f, tap * chans : (tap + n) * chans, :]
            adj = pair.T
            for i in range(n):
                part = slice(i * chans, (i + 1) * chans)
                place(f, tap + i, pair[part].astype(BF16))
                place(f + 2, taps - 1 - tap - i, adj[:, part].astype(BF16))


def strips(r):
    high = r.astype(BF16).astype(F32)
    low = r - high
    upper = lax.broadcasted_iota(jnp.int32, (8, 128), 0) < HALO
    first = jnp.where(upper, high[:8], pltpu.roll(low[:8], HALO, 0))
    last = jnp.where(upper, pltpu.roll(high[-8:], HALO, 0), low[-8:])
    return first.astype(BF16), last.astype(BF16)


def ahead(coef, turns, q, p, n):
    decay, kick, half = coef
    c = turns * half * half * (1.0 + decay)
    return (1.0 - c) * q + half * (1.0 + decay) * p + half * kick * n, c


def prepare_body(coef, r_ref, block_ref, rl_ref, rh_ref):
    for x in range(XB):
        for j in range(4):
            q, p, n = (r_ref[x // 2 * 4 + j, k, x % 2] for k in range(3))
            block_ref[x, j] = q.astype(BF16)
            rl_ref[x, j], rh_ref[x, j] = strips(ahead(coef, 1, q, p, n)[0])


def gradient_body(kind, wide, coef, *refs):
    decay, kick, half = coef
    it = iter(refs)
    r_ref = next(it)
    if kind == "first":
        q_of = lambda x, j: r_ref[x // 2 * 4 + j, 0, x % 2]
        p_of = lambda x, j: r_ref[x // 2 * 4 + j, 1, x % 2]
    else:
        q_ref, p_ref = next(it), next(it)
        q_of = lambda x, j: q_ref[x, j]
        p_of = lambda x, j: p_ref[x, j]
    step_at = {"first": 0}.get(kind, kind)
    noise_of = lambda x, j, k: r_ref[x // 2 * 4 + j, 2 + k, x % 2]
    if wide:
        xl_ref, xh_ref, zl_ref, zh_ref, w_ref, bias_ref = (next(it) for _ in range(6))
    else:
        xl_ref, xh_ref, own_ref, w_ref, bias_ref = (next(it) for _ in range(5))
    if kind == "last":
        out_ref = next(it)
    else:
        qo_ref, po_ref, qb_ref = (next(it) for _ in range(3))
        if not wide:
            rl_ref, rh_ref = next(it), next(it)
    buf, rows_ref, act = (next(it) for _ in range(3))

    pad = 2 * HALO if wide else HALO
    pitch = ZB + 2 * pad
    x_all = XB + 2 * HALO
    lo, hi, end = 8 + pad, 8 + pad + ZB, 8 + pitch
    edge = jnp.zeros((x_all, 4, 8, 128), F32)
    buf[:, :, 0:8, :] = edge
    buf[:, :, end : end + 8, :] = edge
    if wide:
        buf[0:HALO, :, lo:hi, :] = xl_ref[...].astype(F32)
        buf[HALO + XB :, :, lo:hi, :] = xh_ref[...].astype(F32)
        for x in range(XB):
            for j in range(4):
                buf[HALO + x, j, lo:hi, :] = q_of(x, j)
        buf[:, :, 8:lo, :] = zl_ref[0:x_all].astype(F32)
        buf[:, :, hi:end, :] = zh_ref[0:x_all].astype(F32)
    else:
        buf[0:HALO, :, 8:end, :] = xl_ref[...].astype(F32)
        buf[HALO : HALO + XB, :, 8:end, :] = own_ref[...].astype(F32)
        buf[HALO + XB :, :, 8:end, :] = xh_ref[...].astype(F32)

    def conv(x_in, w, use):
        n = x_in * pitch
        for j in range(4):
            for c in range(3):
                v = buf[0:x_in, j, 7 + c : 7 + c + pitch, :].reshape(n, 128).astype(BF16)
                rows_ref[0:n, (j * 3 + c) * 128 : (j * 3 + c + 1) * 128] = v
                if j == 0:
                    rows_ref[0:n, (12 + c) * 128 : (13 + c) * 128] = v
        x_out = x_in - 2
        m = x_out * pitch
        for p in range(4):
            t = jnp.dot(
                rows_ref[0:n, 384 * p : 384 * p + 768], w_ref[w], preferred_element_type=F32
            )
            o = t[0:m, 0:128] + t[pitch : pitch + m, 128:256] + t[2 * pitch :, 256:384]
            use(p, o.reshape(x_out, pitch, 128))

    def hidden(p, h):
        t = jnp.tanh(h + bias_ref[...])
        act[:, p] = 1.0 - t * t
        buf[0 : XB + 6, p, 8:end, :] = t

    def second(p, h):
        buf[0 : XB + 4, p, 8:end, :] = h

    def back(p, g):
        buf[0 : XB + 2, p, 8:end, :] = g * act[2 : XB + 4, (p + 1) % 4]

    def final(p, g):
        buf[0:XB, p, 8:end, :] = g
        j = (p + 2) % 4
        for x in range(XB):
            q = q_of(x, j)
            force = buf[x, p, lo:hi, :] + q
            mom = p_of(x, j) - half * force
            if kind == "last":
                out_ref[x // 2, j, 0, x % 2] = q
                out_ref[x // 2, j, 1, x % 2] = mom
                continue
            if kind != "first":
                mom = mom - half * force
            q = q + half * mom
            mom = decay * mom + kick * noise_of(x, j, step_at)
            q = q + half * mom
            qo_ref[x, j] = q
            po_ref[x, j] = mom
            if not wide:
                qb_ref[x, j] = q.astype(BF16)
                r, _ = ahead(coef, 2, q, mom, noise_of(x, j, step_at + 1))
                rl_ref[x, j], rh_ref[x, j] = strips(r)
                continue
            c = (1 if kind == "first" else 2) * half * half * (1.0 + decay)
            below, above = slice(lo - HALO, lo), slice(hi, hi + HALO)
            for ref, at in ((zl_ref, below), (zh_ref, above)):
                r = ref[x_all + x, j].astype(F32)
                r = r + pltpu.roll(r, HALO, 0)
                buf[x, p, at, :] = r[:HALO] - c * buf[x, p, at, :]
            buf[x, p, lo:hi, :] = q
            qb_ref[x, j] = buf[x, p, lo - HALO : hi + HALO, :].astype(BF16)

    conv(XB + 8, 0, hidden)
    conv(XB + 6, 1, second)
    conv(XB + 4, 3, back)
    conv(XB + 2, 2, final)


def solution(mesh):
    gy, gz = mesh.shape["gy"], mesh.shape["gz"]
    gs = XB // 2
    gX = mesh.shape["gx"] // gs
    fine = Mesh(
        mesh.devices.reshape(mesh.shape["grp"], gX, gs, gy, gz), ("grp", "gX", "gs", "gy", "gz")
    )
    walk = cycle(gs, gy)
    place = [walk.index((a, b)) for a in range(gs) for b in range(gy)]
    ring = [(a * gy + b) * gz + c for c in range(gz) for a, b in walk]

    def x_shift(d):
        return [(i, (i + d) % gX) for i in range(gX)]

    def z_shift(d):
        n = len(ring)
        return [(ring[i], ring[(i + d) % n]) for i in range(n)]

    decay = math.exp(-0.25)
    kick = math.sqrt(1.0 - decay * decay)

    def along_x(block):
        xl = lax.ppermute(block, "gX", x_shift(1))
        xh = lax.ppermute(block, "gX", x_shift(-1))
        return xl, xh

    def along_both(block, rl, rh):
        xl, xh = along_x(block)
        whole = jnp.concatenate([xl, block, xh], axis=0)
        up = jnp.concatenate([whole[:, :, ZB - 2 * HALO :], rh], axis=0)
        down = jnp.concatenate([whole[:, :, : 2 * HALO], rl], axis=0)
        zl = lax.ppermute(up, ("gs", "gy", "gz"), z_shift(1))
        zh = lax.ppermute(down, ("gs", "gy", "gz"), z_shift(-1))
        return xl, xh, zl, zh

    def body(position, momentum, noise, filter_in, filter_out, bias):
        chans = position.shape[0]
        steps = noise.shape[0]
        members = gs * gy

        own = [f.reshape(*f.shape[:2], 27).transpose(0, 2, 1) for f in (filter_in, filter_out)]
        own = jnp.concatenate([f.reshape(f.shape[0], -1) for f in own], axis=1)
        own = jnp.pad(own, ((0, 0), (0, -own.shape[1] % 128)))
        far = lax.all_to_all(
            jnp.broadcast_to(own, (gX, *own.shape)), "gX", 0, 0, tiled=True
        )
        far = far.reshape(-1, far.shape[-1])
        near = lax.all_to_all(
            jnp.broadcast_to(far, (members, *far.shape)), ("gs", "gy"), 0, 0, tiled=True
        )
        near = near.reshape(gs, gy, gX, *own.shape).transpose(1, 2, 0, 3, 4)
        (weights,) = kernel_call(
            weights_body,
            [jax.ShapeDtypeStruct((4, 12 * chans, 6 * chans), BF16)],
            (near.reshape(gy, chans, own.shape[1]),),
            [VMEM((2, 27 * chans, chans), F32)],
        )
        bias_row = jnp.concatenate([bias, bias])[None, :]

        (spread,) = kernel_call(
            functools.partial(spread_body, place),
            [jax.ShapeDtypeStruct((members, 2 + steps, 2, ZB, 128), F32)],
            (position, momentum, noise),
            hbm_in=True,
            hbm_out=True,
        )
        held = lax.all_to_all(spread, ("gs", "gy"), 0, 0, tiled=True)

        coef = (decay, kick, 0.5 * STEP)
        tall = (XB, gy, ZB, 128)
        state32 = jax.ShapeDtypeStruct(tall, F32)
        block16 = jax.ShapeDtypeStruct(tall, BF16)
        grown16 = jax.ShapeDtypeStruct((XB, gy, ZB + 2 * HALO, 128), BF16)
        strip16 = jax.ShapeDtypeStruct((XB, gy, 2 * HALO, 128), BF16)
        block, *ends = kernel_call(
            functools.partial(prepare_body, coef), [block16, strip16, strip16], (held,)
        )
        state = ()
        for k in range(steps + 1):
            kind = "first" if k == 0 else "last" if k == steps else k
            wide = k % 2 == 0
            edges = along_both(block, *ends) if wide else (*along_x(block), block)
            outs = [state32, state32, grown16] if wide else [state32, state32, block16, strip16, strip16]
            if kind == "last":
                outs = [jax.ShapeDtypeStruct((gs, gy, 2, 2, ZB, 128), F32)]
            pitch = ZB + (4 if wide else 2) * HALO
            res = kernel_call(
                functools.partial(gradient_body, kind, wide, coef),
                outs,
                (held, *state, *edges, weights, bias_row),
                (
                    VMEM((XB + 8, gy, pitch + 16, 128), F32),
                    VMEM(((XB + 8) * pitch, 15 * 128), BF16),
                    VMEM((XB + 6, gy, pitch, 128), F32),
                ),
            )
            if kind != "last":
                state, block, ends = tuple(res[:2]), res[2], res[3:]
        back = lax.all_to_all(
            res[0].reshape(members, 2, 2, ZB, 128), ("gs", "gy"), 0, 0, tiled=True
        )
        out = jax.ShapeDtypeStruct(position.shape, F32)
        return tuple(
            kernel_call(functools.partial(collect_body, place), [out, out], (back,), hbm_out=True)
        )

    where = ("grp", "gX", "gs")
    lattice = P(None, where, "gy", "gz")
    filters = P(("gX", "gs"), "gy", None, None, None)
    return jax.shard_map(
        body,
        mesh=fine,
        in_specs=(lattice, lattice, P(None, None, where, "gy", "gz"), filters, filters, P()),
        out_specs=(lattice, lattice),
        check_vma=False,
    )
```

```python
import functools
import math

import jax
import jax.numpy as jnp
from jax import lax
from jax.experimental import pallas as pl
from jax.experimental.pallas import tpu as pltpu
from jax.sharding import Mesh, PartitionSpec as P


F32, BF16 = jnp.float32, jnp.bfloat16
STEP = 0.25
XB, ZB = 4, 16
HALO = 4
VMEM = pltpu.VMEM
LIMIT = 24 * 1024 * 1024


def cycle(rows, cols):
    path = [(0, b) for b in range(cols)]
    for b in range(cols - 1, 0, -1):
        column = [(a, b) for a in range(1, rows)]
        path += column if (cols - 1 - b) % 2 == 0 else column[::-1]
    return path + [(a, 0) for a in range(rows - 1, 0, -1)]


def kernel_call(body, outs, args, scratch=(), hbm_in=False, hbm_out=False):
    spec = pl.BlockSpec(memory_space=VMEM)
    space = pltpu.HBM if hbm_in else VMEM
    args = [pltpu.with_memory_space_constraint(v, space) for v in args]
    return pl.pallas_call(
        body,
        out_shape=outs if hbm_out else [VMEM(o.shape, o.dtype) for o in outs],
        in_specs=[spec] * len(args),
        out_specs=[spec] * len(outs),
        scratch_shapes=list(scratch),
        compiler_params=pltpu.CompilerParams(vmem_limit_bytes=LIMIT),
    )(*args)


def spread_body(place, q_ref, p_ref, n_ref, out_ref):
    def send(part, x, flat):
        for member, block in enumerate(place):
            out_ref[member, part, x] = flat[block * ZB : (block + 1) * ZB, :]

    for x in range(q_ref.shape[1]):
        for k, ref in enumerate((q_ref, p_ref)):
            flat = jnp.concatenate([ref[:, x, y, :] for y in range(ref.shape[2])], axis=0).T
            high = flat.astype(BF16)
            send(2 * k, x, high)
            send(2 * k + 1, x, (flat - high.astype(F32)).astype(BF16))
        for k in range(n_ref.shape[0]):
            parts = [n_ref[k, :, x, y, :].astype(F32) for y in range(n_ref.shape[3])]
            send(4 + k, x, jnp.concatenate(parts, axis=0).T.astype(BF16))


def held_at(r_ref, array, x, j):
    pick = lambda part: r_ref[x // 2 * 4 + j, part, x % 2].astype(F32)
    if array < 2:
        return pick(2 * array) + pick(2 * array + 1)
    return pick(2 + array)


def collect_body(place, in_ref, q_ref, p_ref):
    for k, ref in enumerate((q_ref, p_ref)):
        chans = ref.shape[0]
        for x in range(ref.shape[1]):
            rows = [None] * len(place)
            for member, block in enumerate(place):
                rows[block] = in_ref[member, k, x]
            flat = jnp.concatenate(rows, axis=0).T
            for y in range(ref.shape[2]):
                ref[:, x, y, :] = flat[y * chans : (y + 1) * chans, :]


def weights_body(m_ref, out_ref, fwd_ref):
    groups, chans, _ = m_ref.shape
    per = chans // groups
    taps = 27
    turned = [m_ref[g].astype(F32).T.astype(BF16) for g in range(groups)]
    for f in range(2):
        for tap in range(taps):
            at = (f * taps + tap) * per
            for g in range(groups):
                fwd_ref[f, tap * chans + g * per : tap * chans + (g + 1) * per, :] = turned[g][
                    at : at + per, :
                ].astype(F32)
    zero = jnp.zeros((chans, chans), BF16)

    def place(w, tap, block):
        a, b, c = tap // 9, tap // 3 % 3, tap % 3
        for u in range(2):
            t = b + u
            row = ((t // 2 * 3 + c) * 2 + t % 2) * chans
            col = (a * 2 + u) * chans
            out_ref[w, row : row + chans, col : col + chans] = block

    for w in range(4):
        for c in range(3):
            for a in range(3):
                for t, u in ((3, 0), (0, 1)):
                    row = ((t // 2 * 3 + c) * 2 + t % 2) * chans
                    col = (a * 2 + u) * chans
                    out_ref[w, row : row + chans, col : col + chans] = zero
    for f in range(2):
        for tap in range(0, taps, 2):
            n = min(2, taps - tap)
            pair = fwd_ref[f, tap * chans : (tap + n) * chans, :]
            adj = pair.T
            for i in range(n):
                part = slice(i * chans, (i + 1) * chans)
                place(f, tap + i, pair[part].astype(BF16))
                place(f + 2, taps - 1 - tap - i, adj[:, part].astype(BF16))


def strips(r):
    high = r.astype(BF16).astype(F32)
    low = r - high
    upper = lax.broadcasted_iota(jnp.int32, (8, 128), 0) < HALO
    first = jnp.where(upper, high[:8], pltpu.roll(low[:8], HALO, 0))
    last = jnp.where(upper, pltpu.roll(high[-8:], HALO, 0), low[-8:])
    return first.astype(BF16), last.astype(BF16)


def ahead(coef, turns, q, p, n):
    decay, kick, half = coef
    c = turns * half * half * (1.0 + decay)
    return (1.0 - c) * q + half * (1.0 + decay) * p + half * kick * n, c


def prepare_body(coef, r_ref, block_ref, rl_ref, rh_ref):
    for x in range(XB):
        for j in range(4):
            q, p, n = (held_at(r_ref, k, x, j) for k in range(3))
            block_ref[x, j] = r_ref[x // 2 * 4 + j, 0, x % 2]
            rl_ref[x, j], rh_ref[x, j] = strips(ahead(coef, 1, q, p, n)[0])


def gradient_body(kind, wide, coef, *refs):
    decay, kick, half = coef
    it = iter(refs)
    r_ref = next(it)
    if kind == "first":
        q_of = lambda x, j: held_at(r_ref, 0, x, j)
        p_of = lambda x, j: held_at(r_ref, 1, x, j)
    else:
        q_ref, p_ref = next(it), next(it)
        q_of = lambda x, j: q_ref[x, j]
        p_of = lambda x, j: p_ref[x, j]
    step_at = {"first": 0}.get(kind, kind)
    noise_of = lambda x, j, k: held_at(r_ref, 2 + k, x, j)
    if wide:
        xl_ref, xh_ref, zl_ref, zh_ref, w_ref, bias_ref = (next(it) for _ in range(6))
    else:
        xl_ref, xh_ref, own_ref, w_ref, bias_ref = (next(it) for _ in range(5))
    if kind == "last":
        out_ref = next(it)
    else:
        qo_ref, po_ref, qb_ref = (next(it) for _ in range(3))
        if not wide:
            rl_ref, rh_ref = next(it), next(it)
    buf, rows_ref, act = (next(it) for _ in range(3))

    pad = 2 * HALO if wide else HALO
    pitch = ZB + 2 * pad
    x_all = XB + 2 * HALO
    lo, hi, end = 8 + pad, 8 + pad + ZB, 8 + pitch
    edge = jnp.zeros((x_all, 4, 8, 128), F32)
    buf[:, :, 0:8, :] = edge
    buf[:, :, end : end + 8, :] = edge
    if wide:
        buf[0:HALO, :, lo:hi, :] = xl_ref[...].astype(F32)
        buf[HALO + XB :, :, lo:hi, :] = xh_ref[...].astype(F32)
        for x in range(XB):
            for j in range(4):
                buf[HALO + x, j, lo:hi, :] = q_of(x, j)
        buf[:, :, 8:lo, :] = zl_ref[0:x_all].astype(F32)
        buf[:, :, hi:end, :] = zh_ref[0:x_all].astype(F32)
    else:
        buf[0:HALO, :, 8:end, :] = xl_ref[...].astype(F32)
        buf[HALO : HALO + XB, :, 8:end, :] = own_ref[...].astype(F32)
        buf[HALO + XB :, :, 8:end, :] = xh_ref[...].astype(F32)

    def conv(x_in, w, use):
        n = x_in * pitch
        for j in range(4):
            for c in range(3):
                v = buf[0:x_in, j, 7 + c : 7 + c + pitch, :].reshape(n, 128).astype(BF16)
                rows_ref[0:n, (j * 3 + c) * 128 : (j * 3 + c + 1) * 128] = v
                if j == 0:
                    rows_ref[0:n, (12 + c) * 128 : (13 + c) * 128] = v
        x_out = x_in - 2
        m = x_out * pitch
        for p in range(4):
            cols = slice(384 * p, 384 * p + 768)
            t = jnp.dot(
                rows_ref[0 : n - pitch, cols], w_ref[w, :, 0:256], preferred_element_type=F32
            )
            o = t[0:m, 0:128] + t[pitch:, 128:256]
            o = o + jnp.dot(
                rows_ref[2 * pitch : n, cols], w_ref[w, :, 256:384], preferred_element_type=F32
            )
            use(p, o.reshape(x_out, pitch, 128))

    def hidden(p, h):
        t = jnp.tanh(h + bias_ref[...])
        act[:, p] = 1.0 - t * t
        buf[0 : XB + 6, p, 8:end, :] = t

    def second(p, h):
        buf[0 : XB + 4, p, 8:end, :] = h

    def back(p, g):
        buf[0 : XB + 2, p, 8:end, :] = g * act[2 : XB + 4, (p + 1) % 4]

    def final(p, g):
        buf[0:XB, p, 8:end, :] = g
        j = (p + 2) % 4
        for x in range(XB):
            q = q_of(x, j)
            force = buf[x, p, lo:hi, :] + q
            mom = p_of(x, j) - half * force
            if kind == "last":
                out_ref[x // 2, j, 0, x % 2] = q
                out_ref[x // 2, j, 1, x % 2] = mom
                continue
            if kind != "first":
                mom = mom - half * force
            q = q + half * mom
            mom = decay * mom + kick * noise_of(x, j, step_at)
            q = q + half * mom
            qo_ref[x, j] = q
            po_ref[x, j] = mom
            if not wide:
                qb_ref[x, j] = q.astype(BF16)
                r, _ = ahead(coef, 2, q, mom, noise_of(x, j, step_at + 1))
                rl_ref[x, j], rh_ref[x, j] = strips(r)
                continue
            c = (1 if kind == "first" else 2) * half * half * (1.0 + decay)
            below, above = slice(lo - HALO, lo), slice(hi, hi + HALO)
            for ref, at in ((zl_ref, below), (zh_ref, above)):
                r = ref[x_all + x, j].astype(F32)
                r = r + pltpu.roll(r, HALO, 0)
                buf[x, p, at, :] = r[:HALO] - c * buf[x, p, at, :]
            buf[x, p, lo:hi, :] = q
            qb_ref[x, j] = buf[x, p, lo - HALO : hi + HALO, :].astype(BF16)

    conv(XB + 8, 0, hidden)
    conv(XB + 6, 1, second)
    conv(XB + 4, 3, back)
    conv(XB + 2, 2, final)


def solution(mesh):
    gy, gz = mesh.shape["gy"], mesh.shape["gz"]
    gs = XB // 2
    gX = mesh.shape["gx"] // gs
    fine = Mesh(
        mesh.devices.reshape(mesh.shape["grp"], gX, gs, gy, gz), ("grp", "gX", "gs", "gy", "gz")
    )
    walk = cycle(gs, gy)
    place = [walk.index((a, b)) for a in range(gs) for b in range(gy)]
    ring = [(a * gy + b) * gz + c for c in range(gz) for a, b in walk]

    def x_shift(d):
        return [(i, (i + d) % gX) for i in range(gX)]

    def z_shift(d):
        n = len(ring)
        return [(ring[i], ring[(i + d) % n]) for i in range(n)]

    decay = math.exp(-0.25)
    kick = math.sqrt(1.0 - decay * decay)

    def along_x(block):
        xl = lax.ppermute(block, "gX", x_shift(1))
        xh = lax.ppermute(block, "gX", x_shift(-1))
        return xl, xh

    def along_both(block, rl, rh):
        xl, xh = along_x(block)
        whole = jnp.concatenate([xl, block, xh], axis=0)
        up = jnp.concatenate([whole[:, :, ZB - 2 * HALO :], rh], axis=0)
        down = jnp.concatenate([whole[:, :, : 2 * HALO], rl], axis=0)
        zl = lax.ppermute(up, ("gs", "gy", "gz"), z_shift(1))
        zh = lax.ppermute(down, ("gs", "gy", "gz"), z_shift(-1))
        return xl, xh, zl, zh

    def body(position, momentum, noise, filter_in, filter_out, bias):
        chans = position.shape[0]
        steps = noise.shape[0]
        members = gs * gy

        own = [f.reshape(*f.shape[:2], 27).transpose(0, 2, 1) for f in (filter_in, filter_out)]
        own = jnp.concatenate([f.reshape(f.shape[0], -1) for f in own], axis=1)
        own = jnp.pad(own, ((0, 0), (0, -own.shape[1] % 128)))
        far = lax.all_to_all(
            jnp.broadcast_to(own, (gX, *own.shape)), "gX", 0, 0, tiled=True
        )
        far = far.reshape(-1, far.shape[-1])
        near = lax.all_to_all(
            jnp.broadcast_to(far, (members, *far.shape)), ("gs", "gy"), 0, 0, tiled=True
        )
        near = near.reshape(gs, gy, gX, *own.shape).transpose(1, 2, 0, 3, 4)
        (weights,) = kernel_call(
            weights_body,
            [jax.ShapeDtypeStruct((4, 12 * chans, 6 * chans), BF16)],
            (near.reshape(gy, chans, own.shape[1]),),
            [VMEM((2, 27 * chans, chans), F32)],
        )
        bias_row = jnp.concatenate([bias, bias])[None, :]

        (spread,) = kernel_call(
            functools.partial(spread_body, place),
            [jax.ShapeDtypeStruct((members, 4 + steps, 2, ZB, 128), BF16)],
            (position, momentum, noise),
            hbm_in=True,
            hbm_out=True,
        )
        held = lax.all_to_all(spread, ("gs", "gy"), 0, 0, tiled=True)

        coef = (decay, kick, 0.5 * STEP)
        tall = (XB, gy, ZB, 128)
        state32 = jax.ShapeDtypeStruct(tall, F32)
        block16 = jax.ShapeDtypeStruct(tall, BF16)
        grown16 = jax.ShapeDtypeStruct((XB, gy, ZB + 2 * HALO, 128), BF16)
        strip16 = jax.ShapeDtypeStruct((XB, gy, 2 * HALO, 128), BF16)
        block, *ends = kernel_call(
            functools.partial(prepare_body, coef), [block16, strip16, strip16], (held,)
        )
        state = ()
        for k in range(steps + 1):
            kind = "first" if k == 0 else "last" if k == steps else k
            wide = k % 2 == 0
            edges = along_both(block, *ends) if wide else (*along_x(block), block)
            outs = [state32, state32, grown16] if wide else [state32, state32, block16, strip16, strip16]
            if kind == "last":
                outs = [jax.ShapeDtypeStruct((gs, gy, 2, 2, ZB, 128), F32)]
            pitch = ZB + (4 if wide else 2) * HALO
            res = kernel_call(
                functools.partial(gradient_body, kind, wide, coef),
                outs,
                (held, *state, *edges, weights, bias_row),
                (
                    VMEM((XB + 8, gy, pitch + 16, 128), F32),
                    VMEM(((XB + 8) * pitch, 15 * 128), BF16),
                    VMEM((XB + 6, gy, pitch, 128), F32),
                ),
            )
            if kind != "last":
                state, block, ends = tuple(res[:2]), res[2], res[3:]
        back = lax.all_to_all(
            res[0].reshape(members, 2, 2, ZB, 128), ("gs", "gy"), 0, 0, tiled=True
        )
        out = jax.ShapeDtypeStruct(position.shape, F32)
        return tuple(
            kernel_call(functools.partial(collect_body, place), [out, out], (back,), hbm_out=True)
        )

    where = ("grp", "gX", "gs")
    lattice = P(None, where, "gy", "gz")
    filters = P(("gX", "gs"), "gy", None, None, None)
    return jax.shard_map(
        body,
        mesh=fine,
        in_specs=(lattice, lattice, P(None, None, where, "gy", "gz"), filters, filters, P()),
        out_specs=(lattice, lattice),
        check_vma=False,
    )
```

```python
import functools
import math

import jax
import jax.numpy as jnp
from jax import lax
from jax.experimental import pallas as pl
from jax.experimental.pallas import tpu as pltpu
from jax.sharding import Mesh, PartitionSpec as P


F32, BF16 = jnp.float32, jnp.bfloat16
STEP = 0.25
XB, ZB = 4, 16
HALO = 4
VMEM = pltpu.VMEM
LIMIT = 24 * 1024 * 1024


def cycle(rows, cols):
    path = [(0, b) for b in range(cols)]
    for b in range(cols - 1, 0, -1):
        column = [(a, b) for a in range(1, rows)]
        path += column if (cols - 1 - b) % 2 == 0 else column[::-1]
    return path + [(a, 0) for a in range(rows - 1, 0, -1)]


def kernel_call(body, outs, args, scratch=(), hbm_in=False, hbm_out=False):
    spec = pl.BlockSpec(memory_space=VMEM)
    space = pltpu.HBM if hbm_in else VMEM
    args = [pltpu.with_memory_space_constraint(v, space) for v in args]
    return pl.pallas_call(
        body,
        out_shape=outs if hbm_out else [VMEM(o.shape, o.dtype) for o in outs],
        in_specs=[spec] * len(args),
        out_specs=[spec] * len(outs),
        scratch_shapes=list(scratch),
        compiler_params=pltpu.CompilerParams(vmem_limit_bytes=LIMIT),
    )(*args)


def spread_body(place, q_ref, p_ref, n_ref, out_ref):
    def send(part, x, flat):
        for member, block in enumerate(place):
            out_ref[member, part, x] = flat[block * ZB : (block + 1) * ZB, :]

    for x in range(q_ref.shape[1]):
        for k, ref in enumerate((q_ref, p_ref)):
            flat = jnp.concatenate([ref[:, x, y, :] for y in range(ref.shape[2])], axis=0).T
            high = flat.astype(BF16)
            send(2 * k, x, high)
            send(2 * k + 1, x, (flat - high.astype(F32)).astype(BF16))
        for k in range(n_ref.shape[0]):
            parts = [n_ref[k, :, x, y, :].astype(F32) for y in range(n_ref.shape[3])]
            send(4 + k, x, jnp.concatenate(parts, axis=0).T.astype(BF16))


def held_at(r_ref, array, x, j):
    pick = lambda part: r_ref[x // 2 * 4 + j, part, x % 2].astype(F32)
    if array < 2:
        return pick(2 * array) + pick(2 * array + 1)
    return pick(2 + array)


def collect_body(place, in_ref, q_ref, p_ref):
    for k, ref in enumerate((q_ref, p_ref)):
        chans = ref.shape[0]
        for x in range(ref.shape[1]):
            rows = [None] * len(place)
            for member, block in enumerate(place):
                rows[block] = in_ref[member, k, x]
            flat = jnp.concatenate(rows, axis=0).T
            for y in range(ref.shape[2]):
                ref[:, x, y, :] = flat[y * chans : (y + 1) * chans, :]


def weights_body(near, m_ref, out_ref, fwd_ref):
    groups = near[1]
    chans = near[0] * m_ref.shape[1]
    per = chans // groups
    taps = 27
    at = lax.broadcasted_iota(jnp.int32, (chans, chans), 0)
    row = at % (2 * near[0]) // 2 * (chans // near[0]) + at // (2 * near[0]) * 2 + at % 2
    swap = (row == lax.broadcasted_iota(jnp.int32, (chans, chans), 1)).astype(BF16)
    turned = []
    for g in range(groups):
        m = jnp.concatenate([m_ref[a * groups + g] for a in range(near[0])], axis=0)
        m = jnp.dot(swap, m, preferred_element_type=F32)
        turned.append(m.T.astype(BF16))
    for f in range(2):
        for tap in range(taps):
            at = (f * taps + tap) * per
            for g in range(groups):
                fwd_ref[f, tap * chans + g * per : tap * chans + (g + 1) * per, :] = turned[g][
                    at : at + per, :
                ].astype(F32)
    zero = jnp.zeros((chans, chans), BF16)

    def place(w, tap, block):
        a, b, c = tap // 9, tap // 3 % 3, tap % 3
        for u in range(2):
            t = b + u
            row = ((t // 2 * 3 + c) * 2 + t % 2) * chans
            col = (a * 2 + u) * chans
            out_ref[w, row : row + chans, col : col + chans] = block

    for w in range(4):
        for c in range(3):
            for a in range(3):
                for t, u in ((3, 0), (0, 1)):
                    row = ((t // 2 * 3 + c) * 2 + t % 2) * chans
                    col = (a * 2 + u) * chans
                    out_ref[w, row : row + chans, col : col + chans] = zero
    for f in range(2):
        for tap in range(0, taps, 2):
            n = min(2, taps - tap)
            pair = fwd_ref[f, tap * chans : (tap + n) * chans, :]
            adj = pair.T
            for i in range(n):
                part = slice(i * chans, (i + 1) * chans)
                place(f, tap + i, pair[part].astype(BF16))
                place(f + 2, taps - 1 - tap - i, adj[:, part].astype(BF16))


def strips(r):
    high = r.astype(BF16).astype(F32)
    low = r - high
    upper = lax.broadcasted_iota(jnp.int32, (8, 128), 0) < HALO
    first = jnp.where(upper, high[:8], pltpu.roll(low[:8], HALO, 0))
    last = jnp.where(upper, pltpu.roll(high[-8:], HALO, 0), low[-8:])
    return first.astype(BF16), last.astype(BF16)


def ahead(coef, turns, q, p, n):
    decay, kick, half = coef
    c = turns * half * half * (1.0 + decay)
    return (1.0 - c) * q + half * (1.0 + decay) * p + half * kick * n, c


def prepare_body(coef, r_ref, block_ref, rl_ref, rh_ref):
    for x in range(XB):
        for j in range(4):
            q, p, n = (held_at(r_ref, k, x, j) for k in range(3))
            block_ref[x, j] = r_ref[x // 2 * 4 + j, 0, x % 2]
            rl_ref[x, j], rh_ref[x, j] = strips(ahead(coef, 1, q, p, n)[0])


def gradient_body(kind, wide, coef, *refs):
    decay, kick, half = coef
    it = iter(refs)
    r_ref = next(it)
    if kind == "first":
        q_of = lambda x, j: held_at(r_ref, 0, x, j)
        p_of = lambda x, j: held_at(r_ref, 1, x, j)
    else:
        q_ref, p_ref = next(it), next(it)
        q_of = lambda x, j: q_ref[x, j]
        p_of = lambda x, j: p_ref[x, j]
    step_at = {"first": 0}.get(kind, kind)
    noise_of = lambda x, j, k: held_at(r_ref, 2 + k, x, j)
    if wide:
        xl_ref, xh_ref, zl_ref, zh_ref, w_ref, bias_ref = (next(it) for _ in range(6))
    else:
        xl_ref, xh_ref, own_ref, w_ref, bias_ref = (next(it) for _ in range(5))
    if kind == "last":
        out_ref = next(it)
    else:
        qo_ref, po_ref, qb_ref = (next(it) for _ in range(3))
        if not wide:
            rl_ref, rh_ref = next(it), next(it)
    buf, rows_a, rows_b, act = (next(it) for _ in range(4))

    pad = 2 * HALO if wide else HALO
    pitch = ZB + 2 * pad
    x_all = XB + 2 * HALO
    lo, hi, end = 8 + pad, 8 + pad + ZB, 8 + pitch
    edge = jnp.zeros((x_all, 4, 8, 128), F32)
    buf[:, :, 0:8, :] = edge
    buf[:, :, end : end + 8, :] = edge
    if wide:
        buf[0:HALO, :, lo:hi, :] = xl_ref[...].astype(F32)
        buf[HALO + XB :, :, lo:hi, :] = xh_ref[...].astype(F32)
        for x in range(XB):
            for j in range(4):
                buf[HALO + x, j, lo:hi, :] = q_of(x, j)
        buf[:, :, 8:lo, :] = zl_ref[0:x_all].astype(F32)
        buf[:, :, hi:end, :] = zh_ref[0:x_all].astype(F32)
    else:
        buf[0:HALO, :, 8:end, :] = xl_ref[...].astype(F32)
        buf[HALO : HALO + XB, :, 8:end, :] = own_ref[...].astype(F32)
        buf[HALO + XB :, :, 8:end, :] = xh_ref[...].astype(F32)

    def build(j, x_in, rows):
        n = x_in * pitch
        for c in range(3):
            v = buf[0:x_in, j, 7 + c : 7 + c + pitch, :].reshape(n, 128).astype(BF16)
            rows[0:n, (j * 3 + c) * 128 : (j * 3 + c + 1) * 128] = v
            if j == 0:
                rows[0:n, (12 + c) * 128 : (13 + c) * 128] = v

    def conv(x_in, w, use, rows, then=None):
        n = x_in * pitch
        x_out = x_in - 2
        m = x_out * pitch
        for p in range(4):
            cols = slice(384 * p, 384 * p + 768)
            t = jnp.dot(rows[0 : n - pitch, cols], w_ref[w, :, 0:256], preferred_element_type=F32)
            o = t[0:m, 0:128] + t[pitch:, 128:256]
            o = o + jnp.dot(
                rows[2 * pitch : n, cols], w_ref[w, :, 256:384], preferred_element_type=F32
            )
            use(p, o.reshape(x_out, pitch, 128))
            if then is not None:
                build(p, x_out, then)

    def hidden(p, h):
        t = jnp.tanh(h + bias_ref[...])
        act[:, p] = 1.0 - t * t
        buf[0 : XB + 6, p, 8:end, :] = t

    def second(p, h):
        buf[0 : XB + 4, p, 8:end, :] = h

    def back(p, g):
        buf[0 : XB + 2, p, 8:end, :] = g * act[2 : XB + 4, (p + 1) % 4]

    def final(p, g):
        buf[0:XB, p, 8:end, :] = g
        j = (p + 2) % 4
        for x in range(XB):
            q = q_of(x, j)
            force = buf[x, p, lo:hi, :] + q
            mom = p_of(x, j) - half * force
            if kind == "last":
                out_ref[x // 2, j, 0, x % 2] = q
                out_ref[x // 2, j, 1, x % 2] = mom
                continue
            if kind != "first":
                mom = mom - half * force
            q = q + half * mom
            mom = decay * mom + kick * noise_of(x, j, step_at)
            q = q + half * mom
            qo_ref[x, j] = q
            po_ref[x, j] = mom
            if not wide:
                qb_ref[x, j] = q.astype(BF16)
                r, _ = ahead(coef, 2, q, mom, noise_of(x, j, step_at + 1))
                rl_ref[x, j], rh_ref[x, j] = strips(r)
                continue
            c = (1 if kind == "first" else 2) * half * half * (1.0 + decay)
            below, above = slice(lo - HALO, lo), slice(hi, hi + HALO)
            for ref, at in ((zl_ref, below), (zh_ref, above)):
                r = ref[x_all + x, j].astype(F32)
                r = r + pltpu.roll(r, HALO, 0)
                buf[x, p, at, :] = r[:HALO] - c * buf[x, p, at, :]
            buf[x, p, lo:hi, :] = q
            qb_ref[x, j] = buf[x, p, lo - HALO : hi + HALO, :].astype(BF16)

    for j in range(4):
        build(j, XB + 8, rows_a)
    conv(XB + 8, 0, hidden, rows_a, rows_b)
    conv(XB + 6, 1, second, rows_b, rows_a)
    conv(XB + 4, 3, back, rows_a, rows_b)
    conv(XB + 2, 2, final, rows_b)


def solution(mesh):
    gy, gz = mesh.shape["gy"], mesh.shape["gz"]
    gs = XB // 2
    gX = mesh.shape["gx"] // gs
    fine = Mesh(
        mesh.devices.reshape(mesh.shape["grp"], gX, gs, gy, gz), ("grp", "gX", "gs", "gy", "gz")
    )
    walk = cycle(gs, gy)
    place = [walk.index((a, b)) for a in range(gs) for b in range(gy)]
    ring = [(a * gy + b) * gz + c for c in range(gz) for a, b in walk]

    def x_shift(d):
        return [(i, (i + d) % gX) for i in range(gX)]

    def z_shift(d):
        n = len(ring)
        return [(ring[i], ring[(i + d) % n]) for i in range(n)]

    decay = math.exp(-0.25)
    kick = math.sqrt(1.0 - decay * decay)

    def along_x(block):
        xl = lax.ppermute(block, "gX", x_shift(1))
        xh = lax.ppermute(block, "gX", x_shift(-1))
        return xl, xh

    def along_both(block, rl, rh):
        xl, xh = along_x(block)
        whole = jnp.concatenate([xl, block, xh], axis=0)
        up = jnp.concatenate([whole[:, :, ZB - 2 * HALO :], rh], axis=0)
        down = jnp.concatenate([whole[:, :, : 2 * HALO], rl], axis=0)
        zl = lax.ppermute(up, ("gs", "gy", "gz"), z_shift(1))
        zh = lax.ppermute(down, ("gs", "gy", "gz"), z_shift(-1))
        return xl, xh, zl, zh

    def body(position, momentum, noise, filter_in, filter_out, bias):
        chans = position.shape[0]
        steps = noise.shape[0]
        members = gs * gy

        own = [f.reshape(*f.shape[:2], 27).transpose(0, 2, 1) for f in (filter_in, filter_out)]
        own = jnp.concatenate([f.reshape(f.shape[0], -1) for f in own], axis=1)
        own = jnp.pad(own, ((0, 0), (0, -own.shape[1] % 128)))
        far = lax.all_to_all(
            jnp.broadcast_to(own, (gX, *own.shape)), "gX", 0, 0, tiled=True
        )
        far = far.reshape(-1, far.shape[-1])
        near = lax.all_to_all(
            jnp.broadcast_to(far, (members, *far.shape)), ("gs", "gy"), 0, 0, tiled=True
        )
        (weights,) = kernel_call(
            functools.partial(weights_body, (gs, gy)),
            [jax.ShapeDtypeStruct((4, 12 * chans, 6 * chans), BF16)],
            (near,),
            [VMEM((2, 27 * chans, chans), F32)],
        )
        bias_row = jnp.concatenate([bias, bias])[None, :]

        (spread,) = kernel_call(
            functools.partial(spread_body, place),
            [jax.ShapeDtypeStruct((members, 4 + steps, 2, ZB, 128), BF16)],
            (position, momentum, noise),
            hbm_in=True,
            hbm_out=True,
        )
        held = lax.all_to_all(spread, ("gs", "gy"), 0, 0, tiled=True)

        coef = (decay, kick, 0.5 * STEP)
        tall = (XB, gy, ZB, 128)
        state32 = jax.ShapeDtypeStruct(tall, F32)
        block16 = jax.ShapeDtypeStruct(tall, BF16)
        grown16 = jax.ShapeDtypeStruct((XB, gy, ZB + 2 * HALO, 128), BF16)
        strip16 = jax.ShapeDtypeStruct((XB, gy, 2 * HALO, 128), BF16)
        block, *ends = kernel_call(
            functools.partial(prepare_body, coef), [block16, strip16, strip16], (held,)
        )
        state = ()
        for k in range(steps + 1):
            kind = "first" if k == 0 else "last" if k == steps else k
            wide = k % 2 == 0
            edges = along_both(block, *ends) if wide else (*along_x(block), block)
            outs = [state32, state32, grown16] if wide else [state32, state32, block16, strip16, strip16]
            if kind == "last":
                outs = [jax.ShapeDtypeStruct((gs, gy, 2, 2, ZB, 128), F32)]
            pitch = ZB + (4 if wide else 2) * HALO
            res = kernel_call(
                functools.partial(gradient_body, kind, wide, coef),
                outs,
                (held, *state, *edges, weights, bias_row),
                (
                    VMEM((XB + 8, gy, pitch + 16, 128), F32),
                    VMEM(((XB + 8) * pitch, 15 * 128), BF16),
                    VMEM(((XB + 6) * pitch, 15 * 128), BF16),
                    VMEM((XB + 6, gy, pitch, 128), F32),
                ),
            )
            if kind != "last":
                state, block, ends = tuple(res[:2]), res[2], res[3:]
        back = lax.all_to_all(
            res[0].reshape(members, 2, 2, ZB, 128), ("gs", "gy"), 0, 0, tiled=True
        )
        out = jax.ShapeDtypeStruct(position.shape, F32)
        return tuple(
            kernel_call(functools.partial(collect_body, place), [out, out], (back,), hbm_out=True)
        )

    where = ("grp", "gX", "gs")
    lattice = P(None, where, "gy", "gz")
    filters = P(("gX", "gs"), "gy", None, None, None)
    return jax.shard_map(
        body,
        mesh=fine,
        in_specs=(lattice, lattice, P(None, None, where, "gy", "gz"), filters, filters, P()),
        out_specs=(lattice, lattice),
        check_vma=False,
    )
```

```python
import functools
import math

import jax
import jax.numpy as jnp
from jax import lax
from jax.experimental import pallas as pl
from jax.experimental.pallas import tpu as pltpu
from jax.sharding import Mesh, PartitionSpec as P


F32, BF16 = jnp.float32, jnp.bfloat16
STEP = 0.25
XB, ZB = 4, 16
HALO = 4
VMEM = pltpu.VMEM
LIMIT = 24 * 1024 * 1024


def cycle(rows, cols):
    path = [(0, b) for b in range(cols)]
    for b in range(cols - 1, 0, -1):
        column = [(a, b) for a in range(1, rows)]
        path += column if (cols - 1 - b) % 2 == 0 else column[::-1]
    return path + [(a, 0) for a in range(rows - 1, 0, -1)]


def kernel_call(body, outs, args, scratch=(), hbm_in=False, hbm_out=False, out_space=VMEM):
    spec = pl.BlockSpec(memory_space=VMEM)
    space = pltpu.HBM if hbm_in else VMEM
    args = [pltpu.with_memory_space_constraint(v, space) for v in args]
    return pl.pallas_call(
        body,
        out_shape=outs if hbm_out else [VMEM(o.shape, o.dtype) for o in outs],
        in_specs=[spec] * len(args),
        out_specs=[pl.BlockSpec(memory_space=out_space)] * len(outs),
        scratch_shapes=list(scratch),
        compiler_params=pltpu.CompilerParams(vmem_limit_bytes=LIMIT),
    )(*args)


def spread_body(place, q_ref, p_ref, n_ref, out_ref, made, sems):
    copies = []

    def keep(part, x, flat):
        for member, block in enumerate(place):
            made[member, part, x] = flat[block * ZB : (block + 1) * ZB, :]

    def send(part):
        copies.append(pltpu.make_async_copy(made.at[:, part], out_ref.at[:, part], sems.at[part]))
        copies[-1].start()

    for k, ref in enumerate((q_ref, p_ref)):
        for x in range(ref.shape[1]):
            flat = jnp.concatenate([ref[:, x, y, :] for y in range(ref.shape[2])], axis=0).T
            high = flat.astype(BF16)
            keep(2 * k, x, high)
            keep(2 * k + 1, x, (flat - high.astype(F32)).astype(BF16))
        send(2 * k)
        send(2 * k + 1)
    for k in range(n_ref.shape[0]):
        for x in range(n_ref.shape[2]):
            parts = [n_ref[k, :, x, y, :].astype(F32) for y in range(n_ref.shape[3])]
            keep(4 + k, x, jnp.concatenate(parts, axis=0).T.astype(BF16))
        send(4 + k)
    for copy in copies:
        copy.wait()


def held_at(r_ref, array, x, j):
    pick = lambda part: r_ref[x // 2 * 4 + j, part, x % 2].astype(F32)
    if array < 2:
        return pick(2 * array) + pick(2 * array + 1)
    return pick(2 + array)


def collect_body(place, in_ref, q_ref, p_ref):
    for k, ref in enumerate((q_ref, p_ref)):
        chans = ref.shape[0]
        for x in range(ref.shape[1]):
            rows = [None] * len(place)
            for member, block in enumerate(place):
                rows[block] = in_ref[member, k, x]
            flat = jnp.concatenate(rows, axis=0).T
            for y in range(ref.shape[2]):
                ref[:, x, y, :] = flat[y * chans : (y + 1) * chans, :]


def weights_body(near, m_ref, out_ref, top_ref, fwd_ref):
    groups = near[1]
    chans = near[0] * m_ref.shape[1]
    per = chans // groups
    taps = 27
    at = lax.broadcasted_iota(jnp.int32, (chans, chans), 0)
    row = at % (2 * near[0]) // 2 * (chans // near[0]) + at // (2 * near[0]) * 2 + at % 2
    swap = (row == lax.broadcasted_iota(jnp.int32, (chans, chans), 1)).astype(BF16)
    turned = []
    for g in range(groups):
        m = jnp.concatenate([m_ref[a * groups + g] for a in range(near[0])], axis=0)
        m = jnp.dot(swap, m, preferred_element_type=F32)
        turned.append(m.T.astype(BF16))
    for f in range(2):
        for tap in range(taps):
            at = (f * taps + tap) * per
            for g in range(groups):
                fwd_ref[f, tap * chans + g * per : tap * chans + (g + 1) * per, :] = turned[g][
                    at : at + per, :
                ].astype(F32)
    zero = jnp.zeros((chans, chans), BF16)

    def store(w, a, row, u, block):
        row = row * chans
        if a < 2:
            col = (a * 2 + u) * chans
            out_ref[w, row : row + chans, col : col + chans] = block
            return
        for pair in range(2):
            at, col = row + pair * 6 * chans, (pair * 2 + u) * chans
            top_ref[w, at : at + chans, col : col + chans] = block

    def place(w, tap, block):
        a, b, c = tap // 9, tap // 3 % 3, tap % 3
        for u in range(2):
            t = b + u
            store(w, a, (t // 2 * 3 + c) * 2 + t % 2, u, block)

    for w in range(4):
        top_ref[w, 0 : 6 * chans, 2 * chans :] = jnp.zeros((6 * chans, 2 * chans), BF16)
        top_ref[w, 12 * chans :, 0 : 2 * chans] = jnp.zeros((6 * chans, 2 * chans), BF16)
        for c in range(3):
            for a in range(3):
                for t, u in ((3, 0), (0, 1)):
                    store(w, a, (t // 2 * 3 + c) * 2 + t % 2, u, zero)
    for f in range(2):
        for tap in range(0, taps, 2):
            n = min(2, taps - tap)
            pair = fwd_ref[f, tap * chans : (tap + n) * chans, :]
            adj = pair.T
            for i in range(n):
                part = slice(i * chans, (i + 1) * chans)
                place(f, tap + i, pair[part].astype(BF16))
                place(f + 2, taps - 1 - tap - i, adj[:, part].astype(BF16))


def strips(r):
    high = r.astype(BF16).astype(F32)
    low = r - high
    upper = lax.broadcasted_iota(jnp.int32, (8, 128), 0) < HALO
    first = jnp.where(upper, high[:8], pltpu.roll(low[:8], HALO, 0))
    last = jnp.where(upper, pltpu.roll(high[-8:], HALO, 0), low[-8:])
    return first.astype(BF16), last.astype(BF16)


def ahead(coef, turns, q, p, n):
    decay, kick, half = coef
    c = turns * half * half * (1.0 + decay)
    return (1.0 - c) * q + half * (1.0 + decay) * p + half * kick * n, c


def prepare_body(coef, r_ref, block_ref, rl_ref, rh_ref):
    for x in range(XB):
        for j in range(4):
            q, p, n = (held_at(r_ref, k, x, j) for k in range(3))
            block_ref[x, j] = r_ref[x // 2 * 4 + j, 0, x % 2]
            rl_ref[x, j], rh_ref[x, j] = strips(ahead(coef, 1, q, p, n)[0])


def gradient_body(kind, wide, coef, *refs):
    decay, kick, half = coef
    it = iter(refs)
    r_ref = next(it)
    if kind == "first":
        q_of = lambda x, j: held_at(r_ref, 0, x, j)
        p_of = lambda x, j: held_at(r_ref, 1, x, j)
    else:
        q_ref, p_ref = next(it), next(it)
        q_of = lambda x, j: q_ref[x, j]
        p_of = lambda x, j: p_ref[x, j]
    step_at = {"first": 0}.get(kind, kind)
    noise_of = lambda x, j, k: held_at(r_ref, 2 + k, x, j)
    if wide:
        xl_ref, xh_ref, zl_ref, zh_ref, w_ref, w2_ref, bias_ref = (next(it) for _ in range(7))
    else:
        xl_ref, xh_ref, own_ref, w_ref, w2_ref, bias_ref = (next(it) for _ in range(6))
    if kind == "last":
        out_ref = next(it)
    else:
        qo_ref, po_ref, qb_ref = (next(it) for _ in range(3))
        if not wide:
            rl_ref, rh_ref = next(it), next(it)
    buf, rows_a, rows_b, act = (next(it) for _ in range(4))

    pad = 2 * HALO if wide else HALO
    pitch = ZB + 2 * pad
    x_all = XB + 2 * HALO
    lo, hi, end = 8 + pad, 8 + pad + ZB, 8 + pitch
    edge = jnp.zeros((x_all, 4, 8, 128), F32)
    buf[:, :, 0:8, :] = edge
    buf[:, :, end : end + 8, :] = edge
    if wide:
        buf[0:HALO, :, lo:hi, :] = xl_ref[...].astype(F32)
        buf[HALO + XB :, :, lo:hi, :] = xh_ref[...].astype(F32)
        for x in range(XB):
            for j in range(4):
                buf[HALO + x, j, lo:hi, :] = q_of(x, j)
        buf[:, :, 8:lo, :] = zl_ref[0:x_all].astype(F32)
        buf[:, :, hi:end, :] = zh_ref[0:x_all].astype(F32)
    else:
        buf[0:HALO, :, 8:end, :] = xl_ref[...].astype(F32)
        buf[HALO : HALO + XB, :, 8:end, :] = own_ref[...].astype(F32)
        buf[HALO + XB :, :, 8:end, :] = xh_ref[...].astype(F32)

    def build(j, x_in, rows):
        n = x_in * pitch
        for c in range(3):
            v = buf[0:x_in, j, 7 + c : 7 + c + pitch, :].reshape(n, 128).astype(BF16)
            rows[0:n, (j * 3 + c) * 128 : (j * 3 + c + 1) * 128] = v
            if j == 0:
                rows[0:n, (12 + c) * 128 : (13 + c) * 128] = v

    def conv(x_in, w, use, rows, then=None):
        n = x_in * pitch
        x_out = x_in - 2
        m = x_out * pitch
        for p in range(4):
            cols = slice(384 * p, 384 * p + 768)
            t = jnp.dot(rows[0 : n - pitch, cols], w_ref[w], preferred_element_type=F32)
            if p % 2 == 0:
                cols = slice(384 * p, 384 * p + 1152)
                top = jnp.dot(rows[2 * pitch : n, cols], w2_ref[w], preferred_element_type=F32)
            o = t[0:m, 0:128] + t[pitch:, 128:256] + top[:, p % 2 * 128 : p % 2 * 128 + 128]
            use(p, o.reshape(x_out, pitch, 128))
            if then is not None:
                build(p, x_out, then)

    def hidden(p, h):
        t = jnp.tanh(h + bias_ref[...])
        act[:, p] = 1.0 - t * t
        buf[0 : XB + 6, p, 8:end, :] = t

    def second(p, h):
        buf[0 : XB + 4, p, 8:end, :] = h

    def back(p, g):
        buf[0 : XB + 2, p, 8:end, :] = g * act[2 : XB + 4, (p + 1) % 4]

    def final(p, g):
        buf[0:XB, p, 8:end, :] = g
        j = (p + 2) % 4
        for x in range(XB):
            q = q_of(x, j)
            force = buf[x, p, lo:hi, :] + q
            mom = p_of(x, j) - half * force
            if kind == "last":
                out_ref[x // 2, j, 0, x % 2] = q
                out_ref[x // 2, j, 1, x % 2] = mom
                continue
            if kind != "first":
                mom = mom - half * force
            q = q + half * mom
            mom = decay * mom + kick * noise_of(x, j, step_at)
            q = q + half * mom
            qo_ref[x, j] = q
            po_ref[x, j] = mom
            if not wide:
                qb_ref[x, j] = q.astype(BF16)
                r, _ = ahead(coef, 2, q, mom, noise_of(x, j, step_at + 1))
                rl_ref[x, j], rh_ref[x, j] = strips(r)
                continue
            c = (1 if kind == "first" else 2) * half * half * (1.0 + decay)
            below, above = slice(lo - HALO, lo), slice(hi, hi + HALO)
            for ref, at in ((zl_ref, below), (zh_ref, above)):
                r = ref[x_all + x, j].astype(F32)
                r = r + pltpu.roll(r, HALO, 0)
                buf[x, p, at, :] = r[:HALO] - c * buf[x, p, at, :]
            buf[x, p, lo:hi, :] = q
            qb_ref[x, j] = buf[x, p, lo - HALO : hi + HALO, :].astype(BF16)

    for j in range(4):
        build(j, XB + 8, rows_a)
    conv(XB + 8, 0, hidden, rows_a, rows_b)
    conv(XB + 6, 1, second, rows_b, rows_a)
    conv(XB + 4, 3, back, rows_a, rows_b)
    conv(XB + 2, 2, final, rows_b)


def solution(mesh):
    gy, gz = mesh.shape["gy"], mesh.shape["gz"]
    gs = XB // 2
    gX = mesh.shape["gx"] // gs
    fine = Mesh(
        mesh.devices.reshape(mesh.shape["grp"], gX, gs, gy, gz), ("grp", "gX", "gs", "gy", "gz")
    )
    walk = cycle(gs, gy)
    place = [walk.index((a, b)) for a in range(gs) for b in range(gy)]
    ring = [(a * gy + b) * gz + c for c in range(gz) for a, b in walk]

    def x_shift(d):
        return [(i, (i + d) % gX) for i in range(gX)]

    def z_shift(d):
        n = len(ring)
        return [(ring[i], ring[(i + d) % n]) for i in range(n)]

    decay = math.exp(-0.25)
    kick = math.sqrt(1.0 - decay * decay)

    def along_x(block):
        xl = lax.ppermute(block, "gX", x_shift(1))
        xh = lax.ppermute(block, "gX", x_shift(-1))
        return xl, xh

    def along_both(block, rl, rh):
        xl, xh = along_x(block)
        whole = jnp.concatenate([xl, block, xh], axis=0)
        up = jnp.concatenate([whole[:, :, ZB - 2 * HALO :], rh], axis=0)
        down = jnp.concatenate([whole[:, :, : 2 * HALO], rl], axis=0)
        zl = lax.ppermute(up, ("gs", "gy", "gz"), z_shift(1))
        zh = lax.ppermute(down, ("gs", "gy", "gz"), z_shift(-1))
        return xl, xh, zl, zh

    def body(position, momentum, noise, filter_in, filter_out, bias):
        chans = position.shape[0]
        steps = noise.shape[0]
        members = gs * gy

        own = [f.reshape(*f.shape[:2], 27).transpose(0, 2, 1) for f in (filter_in, filter_out)]
        own = jnp.concatenate([f.reshape(f.shape[0], -1) for f in own], axis=1)
        own = jnp.pad(own, ((0, 0), (0, -own.shape[1] % 128)))
        far = lax.all_to_all(
            jnp.broadcast_to(own, (gX, *own.shape)), "gX", 0, 0, tiled=True
        )
        far = far.reshape(-1, far.shape[-1])
        near = lax.all_to_all(
            jnp.broadcast_to(far, (members, *far.shape)), ("gs", "gy"), 0, 0, tiled=True
        )
        weights = kernel_call(
            functools.partial(weights_body, (gs, gy)),
            [
                jax.ShapeDtypeStruct((4, 12 * chans, 4 * chans), BF16),
                jax.ShapeDtypeStruct((4, 18 * chans, 4 * chans), BF16),
            ],
            (near,),
            [VMEM((2, 27 * chans, chans), F32)],
        )
        bias_row = jnp.concatenate([bias, bias])[None, :]

        (spread,) = kernel_call(
            functools.partial(spread_body, place),
            [jax.ShapeDtypeStruct((members, 4 + steps, 2, ZB, 128), BF16)],
            (position, momentum, noise),
            [
                VMEM((members, 4 + steps, 2, ZB, 128), BF16),
                pltpu.SemaphoreType.DMA((4 + steps,)),
            ],
            hbm_in=True,
            hbm_out=True,
            out_space=pl.ANY,
        )
        held = lax.all_to_all(spread, ("gs", "gy"), 0, 0, tiled=True)

        coef = (decay, kick, 0.5 * STEP)
        tall = (XB, gy, ZB, 128)
        state32 = jax.ShapeDtypeStruct(tall, F32)
        block16 = jax.ShapeDtypeStruct(tall, BF16)
        grown16 = jax.ShapeDtypeStruct((XB, gy, ZB + 2 * HALO, 128), BF16)
        strip16 = jax.ShapeDtypeStruct((XB, gy, 2 * HALO, 128), BF16)
        block, *ends = kernel_call(
            functools.partial(prepare_body, coef), [block16, strip16, strip16], (held,)
        )
        state = ()
        for k in range(steps + 1):
            kind = "first" if k == 0 else "last" if k == steps else k
            wide = k % 2 == 0
            edges = along_both(block, *ends) if wide else (*along_x(block), block)
            outs = [state32, state32, grown16] if wide else [state32, state32, block16, strip16, strip16]
            if kind == "last":
                outs = [jax.ShapeDtypeStruct((gs, gy, 2, 2, ZB, 128), F32)]
            pitch = ZB + (4 if wide else 2) * HALO
            res = kernel_call(
                functools.partial(gradient_body, kind, wide, coef),
                outs,
                (held, *state, *edges, *weights, bias_row),
                (
                    VMEM((XB + 8, gy, pitch + 16, 128), F32),
                    VMEM(((XB + 8) * pitch, 15 * 128), BF16),
                    VMEM(((XB + 6) * pitch, 15 * 128), BF16),
                    VMEM((XB + 6, gy, pitch, 128), F32),
                ),
            )
            if kind != "last":
                state, block, ends = tuple(res[:2]), res[2], res[3:]
        back = lax.all_to_all(
            res[0].reshape(members, 2, 2, ZB, 128), ("gs", "gy"), 0, 0, tiled=True
        )
        out = jax.ShapeDtypeStruct(position.shape, F32)
        return tuple(
            kernel_call(functools.partial(collect_body, place), [out, out], (back,), hbm_out=True)
        )

    where = ("grp", "gX", "gs")
    lattice = P(None, where, "gy", "gz")
    filters = P(("gX", "gs"), "gy", None, None, None)
    return jax.shard_map(
        body,
        mesh=fine,
        in_specs=(lattice, lattice, P(None, None, where, "gy", "gz"), filters, filters, P()),
        out_specs=(lattice, lattice),
        check_vma=False,
    )
```

```python
import functools
import math

import jax
import jax.numpy as jnp
from jax import lax
from jax.experimental import pallas as pl
from jax.experimental.pallas import tpu as pltpu
from jax.sharding import Mesh, PartitionSpec as P


F32, BF16 = jnp.float32, jnp.bfloat16
STEP = 0.25
XB, ZB = 4, 16
HALO = 4
VMEM = pltpu.VMEM
LIMIT = 24 * 1024 * 1024


def cycle(rows, cols):
    path = [(0, b) for b in range(cols)]
    for b in range(cols - 1, 0, -1):
        column = [(a, b) for a in range(1, rows)]
        path += column if (cols - 1 - b) % 2 == 0 else column[::-1]
    return path + [(a, 0) for a in range(rows - 1, 0, -1)]


def kernel_call(body, outs, args, scratch=(), hbm_in=False, hbm_out=False, out_space=VMEM):
    spec = pl.BlockSpec(memory_space=VMEM)
    space = pltpu.HBM if hbm_in else VMEM
    args = [pltpu.with_memory_space_constraint(v, space) for v in args]
    return pl.pallas_call(
        body,
        out_shape=outs if hbm_out else [VMEM(o.shape, o.dtype) for o in outs],
        in_specs=[spec] * len(args),
        out_specs=[pl.BlockSpec(memory_space=out_space)] * len(outs),
        scratch_shapes=list(scratch),
        compiler_params=pltpu.CompilerParams(vmem_limit_bytes=LIMIT),
    )(*args)


def spread_body(place, q_ref, p_ref, n_ref, out_ref, made, sems):
    copies = []

    def keep(part, x, flat):
        for member, block in enumerate(place):
            made[member, part, x] = flat[block * ZB : (block + 1) * ZB, :]

    def send(part):
        copies.append(pltpu.make_async_copy(made.at[:, part], out_ref.at[:, part], sems.at[part]))
        copies[-1].start()

    for k, ref in enumerate((q_ref, p_ref)):
        for x in range(ref.shape[1]):
            flat = jnp.concatenate([ref[:, x, y, :] for y in range(ref.shape[2])], axis=0).T
            high = flat.astype(BF16)
            keep(2 * k, x, high)
            keep(2 * k + 1, x, (flat - high.astype(F32)).astype(BF16))
        send(2 * k)
        send(2 * k + 1)
    for k in range(n_ref.shape[0]):
        for x in range(n_ref.shape[2]):
            parts = [n_ref[k, :, x, y, :].astype(F32) for y in range(n_ref.shape[3])]
            keep(4 + k, x, jnp.concatenate(parts, axis=0).T.astype(BF16))
        send(4 + k)
    for copy in copies:
        copy.wait()


def held_at(r_ref, array, x, j):
    pick = lambda part: r_ref[x // 2 * 4 + j, part, x % 2].astype(F32)
    if array < 2:
        return pick(2 * array) + pick(2 * array + 1)
    return pick(2 + array)


def collect_body(place, in_ref, q_ref, p_ref):
    for k, ref in enumerate((q_ref, p_ref)):
        chans = ref.shape[0]
        for x in range(ref.shape[1]):
            rows = [None] * len(place)
            for member, block in enumerate(place):
                rows[block] = in_ref[member, k, x]
            flat = jnp.concatenate(rows, axis=0).T
            for y in range(ref.shape[2]):
                ref[:, x, y, :] = flat[y * chans : (y + 1) * chans, :]


def weights_body(near, m_ref, out_ref, top_ref, fwd_ref):
    groups = near[1]
    chans = near[0] * m_ref.shape[1]
    per = chans // groups
    taps = 27
    at = lax.broadcasted_iota(jnp.int32, (chans, chans), 0)
    row = at % (2 * near[0]) // 2 * (chans // near[0]) + at // (2 * near[0]) * 2 + at % 2
    swap = (row == lax.broadcasted_iota(jnp.int32, (chans, chans), 1)).astype(BF16)
    turned = []
    for g in range(groups):
        m = jnp.concatenate([m_ref[a * groups + g] for a in range(near[0])], axis=0)
        m = jnp.dot(swap, m, preferred_element_type=F32)
        turned.append(m.T.astype(BF16))
    for f in range(2):
        for tap in range(taps):
            at = (f * taps + tap) * per
            for g in range(groups):
                fwd_ref[f, tap * chans + g * per : tap * chans + (g + 1) * per, :] = turned[g][
                    at : at + per, :
                ].astype(F32)
    zero = jnp.zeros((chans, chans), BF16)

    def store(w, a, row, u, block):
        row = row * chans
        if a < 2:
            col = (a * 2 + u) * chans
            out_ref[w, row : row + chans, col : col + chans] = block
            return
        for pair in range(2):
            at, col = row + pair * 6 * chans, (pair * 2 + u) * chans
            top_ref[w, at : at + chans, col : col + chans] = block

    def place(w, tap, block):
        a, b, c = tap // 9, tap // 3 % 3, tap % 3
        for u in range(2):
            t = b + u
            store(w, a, (t // 2 * 3 + c) * 2 + t % 2, u, block)

    for w in range(4):
        top_ref[w, 0 : 6 * chans, 2 * chans :] = jnp.zeros((6 * chans, 2 * chans), BF16)
        top_ref[w, 12 * chans :, 0 : 2 * chans] = jnp.zeros((6 * chans, 2 * chans), BF16)
        for c in range(3):
            for a in range(3):
                for t, u in ((3, 0), (0, 1)):
                    store(w, a, (t // 2 * 3 + c) * 2 + t % 2, u, zero)
    for f in range(2):
        for tap in range(0, taps, 2):
            n = min(2, taps - tap)
            pair = fwd_ref[f, tap * chans : (tap + n) * chans, :]
            adj = pair.T
            for i in range(n):
                part = slice(i * chans, (i + 1) * chans)
                place(f, tap + i, pair[part].astype(BF16))
                place(f + 2, taps - 1 - tap - i, adj[:, part].astype(BF16))


def strips(r):
    high = r.astype(BF16).astype(F32)
    low = r - high
    upper = lax.broadcasted_iota(jnp.int32, (8, 128), 0) < HALO
    first = jnp.where(upper, high[:8], pltpu.roll(low[:8], HALO, 0))
    last = jnp.where(upper, pltpu.roll(high[-8:], HALO, 0), low[-8:])
    return first.astype(BF16), last.astype(BF16)


def ahead(coef, turns, q, p, n):
    decay, kick, half = coef
    c = turns * half * half * (1.0 + decay)
    return (1.0 - c) * q + half * (1.0 + decay) * p + half * kick * n, c


def prepare_body(coef, r_ref, block_ref, rl_ref, rh_ref):
    for x in range(XB):
        for j in range(4):
            q, p, n = (held_at(r_ref, k, x, j) for k in range(3))
            block_ref[x, j] = r_ref[x // 2 * 4 + j, 0, x % 2]
            rl_ref[x, j], rh_ref[x, j] = strips(ahead(coef, 1, q, p, n)[0])


def gradient_body(kind, wide, coef, *refs):
    decay, kick, half = coef
    it = iter(refs)
    r_ref = next(it)
    if kind == "first":
        q_of = lambda x, j: held_at(r_ref, 0, x, j)
        p_of = lambda x, j: held_at(r_ref, 1, x, j)
    else:
        q_ref, p_ref = next(it), next(it)
        q_of = lambda x, j: q_ref[x, j]
        p_of = lambda x, j: p_ref[x, j]
    step_at = {"first": 0}.get(kind, kind)
    noise_of = lambda x, j, k: held_at(r_ref, 2 + k, x, j)
    if wide:
        xl_ref, xh_ref, zl_ref, zh_ref, w_ref, w2_ref, bias_ref = (next(it) for _ in range(7))
    else:
        xl_ref, xh_ref, own_ref, w_ref, w2_ref, bias_ref = (next(it) for _ in range(6))
    if kind == "last":
        out_ref = next(it)
    else:
        qo_ref, po_ref, qb_ref = (next(it) for _ in range(3))
        if not wide:
            rl_ref, rh_ref = next(it), next(it)
    buf, rows_a, rows_b, act = (next(it) for _ in range(4))

    pad = 2 * HALO if wide else HALO
    pitch = ZB + 2 * pad
    x_all = XB + 2 * HALO
    lo, hi, end = 8 + pad, 8 + pad + ZB, 8 + pitch
    edge = jnp.zeros((x_all, 4, 8, 128), F32)
    buf[:, :, 0:8, :] = edge
    buf[:, :, end : end + 8, :] = edge
    if wide:
        buf[0:HALO, :, lo:hi, :] = xl_ref[...].astype(F32)
        buf[HALO + XB :, :, lo:hi, :] = xh_ref[...].astype(F32)
        for x in range(XB):
            for j in range(4):
                buf[HALO + x, j, lo:hi, :] = q_of(x, j)
        buf[:, :, 8:lo, :] = zl_ref[0:x_all].astype(F32)
        buf[:, :, hi:end, :] = zh_ref[0:x_all].astype(F32)
    else:
        buf[0:HALO, :, 8:end, :] = xl_ref[...].astype(F32)
        buf[HALO : HALO + XB, :, 8:end, :] = own_ref[...].astype(F32)
        buf[HALO + XB :, :, 8:end, :] = xh_ref[...].astype(F32)

    def build(j, x_in, rows):
        n = x_in * pitch
        for c in range(3):
            v = buf[0:x_in, j, 7 + c : 7 + c + pitch, :].reshape(n, 128).astype(BF16)
            rows[0:n, (j * 3 + c) * 128 : (j * 3 + c + 1) * 128] = v
            if j == 0:
                rows[0:n, (12 + c) * 128 : (13 + c) * 128] = v

    def conv(x_in, w, use, rows, then=None):
        n = x_in * pitch
        x_out = x_in - 2
        m = x_out * pitch
        for p in range(4):
            cols = slice(384 * p, 384 * p + 768)
            t = jnp.dot(rows[0 : n - pitch, cols], w_ref[w], preferred_element_type=F32)
            if p % 2 == 0:
                cols = slice(384 * p, 384 * p + 1152)
                top = jnp.dot(rows[2 * pitch : n, cols], w2_ref[w], preferred_element_type=F32)
            o = t[0:m, 0:128] + t[pitch:, 128:256] + top[:, p % 2 * 128 : p % 2 * 128 + 128]
            use(p, o.reshape(x_out, pitch, 128))
            if then is not None:
                build(p, x_out, then)

    def hidden(p, h):
        t = jnp.tanh(h + bias_ref[...])
        act[:, p] = 1.0 - t * t
        buf[0 : XB + 6, p, 8:end, :] = t

    def second(p, h):
        buf[0 : XB + 4, p, 8:end, :] = h

    def back(p, g):
        buf[0 : XB + 2, p, 8:end, :] = g * act[2 : XB + 4, (p + 1) % 4]

    def final(p, g):
        buf[0:XB, p, 8:end, :] = g
        j = (p + 2) % 4
        for x in range(XB):
            q = q_of(x, j)
            force = buf[x, p, lo:hi, :] + q
            mom = p_of(x, j) - half * force
            if kind == "last":
                out_ref[x // 2, j, 0, x % 2] = q
                out_ref[x // 2, j, 1, x % 2] = mom
                continue
            if kind != "first":
                mom = mom - half * force
            q = q + half * mom
            mom = decay * mom + kick * noise_of(x, j, step_at)
            q = q + half * mom
            qo_ref[x, j] = q
            po_ref[x, j] = mom
            if not wide:
                qb_ref[x, j] = q.astype(BF16)
                r, _ = ahead(coef, 2, q, mom, noise_of(x, j, step_at + 1))
                rl_ref[x, j], rh_ref[x, j] = strips(r)
                continue
            c = (1 if kind == "first" else 2) * half * half * (1.0 + decay)
            below, above = slice(lo - HALO, lo), slice(hi, hi + HALO)
            for ref, at in ((zl_ref, below), (zh_ref, above)):
                r = ref[x_all + x, j].astype(F32)
                r = r + pltpu.roll(r, HALO, 0)
                buf[x, p, at, :] = r[:HALO] - c * buf[x, p, at, :]
            buf[x, p, lo:hi, :] = q
            qb_ref[x, j] = buf[x, p, lo - HALO : hi + HALO, :].astype(BF16)

    for j in range(4):
        build(j, XB + 8, rows_a)
    conv(XB + 8, 0, hidden, rows_a, rows_b)
    conv(XB + 6, 1, second, rows_b, rows_a)
    conv(XB + 4, 3, back, rows_a, rows_b)
    conv(XB + 2, 2, final, rows_b)


def solution(mesh):
    gy, gz = mesh.shape["gy"], mesh.shape["gz"]
    gs = XB // 2
    gX = mesh.shape["gx"] // gs
    fine = Mesh(
        mesh.devices.reshape(mesh.shape["grp"], gX, gs, gy, gz), ("grp", "gX", "gs", "gy", "gz")
    )
    walk = cycle(gs, gy)
    place = [walk.index((a, b)) for a in range(gs) for b in range(gy)]
    ring = [(a * gy + b) * gz + c for c in range(gz) for a, b in walk]

    def swaps(ring, first):
        n = len(ring)
        pairs = [(ring[i], ring[(i + 1) % n]) for i in range(0 if first else 1, n, 2)]
        return [pair for i, j in pairs for pair in ((i, j), (j, i))]

    def exchange(up, down, axes, ring, even):
        one = up if up is down else jnp.where(even, up, down)
        two = up if up is down else jnp.where(even, down, up)
        one = lax.ppermute(one, axes, swaps(ring, True))
        two = lax.ppermute(two, axes, swaps(ring, False))
        return jnp.where(even, two, one), jnp.where(even, one, two)

    decay = math.exp(-0.25)
    kick = math.sqrt(1.0 - decay * decay)

    def along_x(block):
        even = lax.axis_index("gX") % 2 == 0
        return exchange(block, block, "gX", list(range(gX)), even)

    def along_both(block, rl, rh):
        xl, xh = along_x(block)
        whole = jnp.concatenate([xl, block, xh], axis=0)
        up = jnp.concatenate([whole[:, :, ZB - 2 * HALO :], rh], axis=0)
        down = jnp.concatenate([whole[:, :, : 2 * HALO], rl], axis=0)
        even = (lax.axis_index("gs") + lax.axis_index("gy")) % 2 == 0
        zl, zh = exchange(up, down, ("gs", "gy", "gz"), ring, even)
        return xl, xh, zl, zh

    def body(position, momentum, noise, filter_in, filter_out, bias):
        chans = position.shape[0]
        steps = noise.shape[0]
        members = gs * gy

        own = [f.reshape(*f.shape[:2], 27).transpose(0, 2, 1) for f in (filter_in, filter_out)]
        own = jnp.concatenate([f.reshape(f.shape[0], -1) for f in own], axis=1)
        own = jnp.pad(own, ((0, 0), (0, -own.shape[1] % 128)))
        far = lax.all_to_all(
            jnp.broadcast_to(own, (gX, *own.shape)), "gX", 0, 0, tiled=True
        )
        far = far.reshape(-1, far.shape[-1])
        near = lax.all_to_all(
            jnp.broadcast_to(far, (members, *far.shape)), ("gs", "gy"), 0, 0, tiled=True
        )
        weights = kernel_call(
            functools.partial(weights_body, (gs, gy)),
            [
                jax.ShapeDtypeStruct((4, 12 * chans, 4 * chans), BF16),
                jax.ShapeDtypeStruct((4, 18 * chans, 4 * chans), BF16),
            ],
            (near,),
            [VMEM((2, 27 * chans, chans), F32)],
        )
        bias_row = jnp.concatenate([bias, bias])[None, :]

        (spread,) = kernel_call(
            functools.partial(spread_body, place),
            [jax.ShapeDtypeStruct((members, 4 + steps, 2, ZB, 128), BF16)],
            (position, momentum, noise),
            [
                VMEM((members, 4 + steps, 2, ZB, 128), BF16),
                pltpu.SemaphoreType.DMA((4 + steps,)),
            ],
            hbm_in=True,
            hbm_out=True,
            out_space=pl.ANY,
        )
        held = lax.all_to_all(spread, ("gs", "gy"), 0, 0, tiled=True)

        coef = (decay, kick, 0.5 * STEP)
        tall = (XB, gy, ZB, 128)
        state32 = jax.ShapeDtypeStruct(tall, F32)
        block16 = jax.ShapeDtypeStruct(tall, BF16)
        grown16 = jax.ShapeDtypeStruct((XB, gy, ZB + 2 * HALO, 128), BF16)
        strip16 = jax.ShapeDtypeStruct((XB, gy, 2 * HALO, 128), BF16)
        block, *ends = kernel_call(
            functools.partial(prepare_body, coef), [block16, strip16, strip16], (held,)
        )
        state = ()
        for k in range(steps + 1):
            kind = "first" if k == 0 else "last" if k == steps else k
            wide = k % 2 == 0
            edges = along_both(block, *ends) if wide else (*along_x(block), block)
            outs = [state32, state32, grown16] if wide else [state32, state32, block16, strip16, strip16]
            if kind == "last":
                outs = [jax.ShapeDtypeStruct((gs, gy, 2, 2, ZB, 128), F32)]
            pitch = ZB + (4 if wide else 2) * HALO
            res = kernel_call(
                functools.partial(gradient_body, kind, wide, coef),
                outs,
                (held, *state, *edges, *weights, bias_row),
                (
                    VMEM((XB + 8, gy, pitch + 16, 128), F32),
                    VMEM(((XB + 8) * pitch, 15 * 128), BF16),
                    VMEM(((XB + 6) * pitch, 15 * 128), BF16),
                    VMEM((XB + 6, gy, pitch, 128), F32),
                ),
            )
            if kind != "last":
                state, block, ends = tuple(res[:2]), res[2], res[3:]
        back = lax.all_to_all(
            res[0].reshape(members, 2, 2, ZB, 128), ("gs", "gy"), 0, 0, tiled=True
        )
        out = jax.ShapeDtypeStruct(position.shape, F32)
        return tuple(
            kernel_call(functools.partial(collect_body, place), [out, out], (back,), hbm_out=True)
        )

    where = ("grp", "gX", "gs")
    lattice = P(None, where, "gy", "gz")
    filters = P(("gX", "gs"), "gy", None, None, None)
    return jax.shard_map(
        body,
        mesh=fine,
        in_specs=(lattice, lattice, P(None, None, where, "gy", "gz"), filters, filters, P()),
        out_specs=(lattice, lattice),
        check_vma=False,
    )
```

```python
import functools
import math

import jax
import jax.numpy as jnp
from jax import lax
from jax.experimental import pallas as pl
from jax.experimental.pallas import tpu as pltpu
from jax.sharding import Mesh, PartitionSpec as P


F32, BF16 = jnp.float32, jnp.bfloat16
STEP = 0.25
XB, ZB = 4, 16
HALO = 4
VMEM = pltpu.VMEM
LIMIT = 24 * 1024 * 1024


def cycle(rows, cols):
    path = [(0, b) for b in range(cols)]
    for b in range(cols - 1, 0, -1):
        column = [(a, b) for a in range(1, rows)]
        path += column if (cols - 1 - b) % 2 == 0 else column[::-1]
    return path + [(a, 0) for a in range(rows - 1, 0, -1)]


def kernel_call(body, outs, args, scratch=(), hbm_in=False, hbm_out=False, out_space=VMEM):
    spec = pl.BlockSpec(memory_space=VMEM)
    space = pltpu.HBM if hbm_in else VMEM
    args = [pltpu.with_memory_space_constraint(v, space) for v in args]
    return pl.pallas_call(
        body,
        out_shape=outs if hbm_out else [VMEM(o.shape, o.dtype) for o in outs],
        in_specs=[spec] * len(args),
        out_specs=[pl.BlockSpec(memory_space=out_space)] * len(outs),
        scratch_shapes=list(scratch),
        compiler_params=pltpu.CompilerParams(vmem_limit_bytes=LIMIT),
    )(*args)


def spread_body(place, q_ref, p_ref, n_ref, out_ref, made, sems):
    copies = []

    def keep(part, x, flat):
        for member, block in enumerate(place):
            made[member, part, x] = flat[block * ZB : (block + 1) * ZB, :]

    def send(part):
        copies.append(pltpu.make_async_copy(made.at[:, part], out_ref.at[:, part], sems.at[part]))
        copies[-1].start()

    for k, ref in enumerate((q_ref, p_ref)):
        for x in range(ref.shape[1]):
            flat = jnp.concatenate([ref[:, x, y, :] for y in range(ref.shape[2])], axis=0).T
            high = flat.astype(BF16)
            keep(2 * k, x, high)
            keep(2 * k + 1, x, (flat - high.astype(F32)).astype(BF16))
        send(2 * k)
        send(2 * k + 1)
    for k in range(n_ref.shape[0]):
        for x in range(n_ref.shape[2]):
            parts = [n_ref[k, :, x, y, :].astype(F32) for y in range(n_ref.shape[3])]
            keep(4 + k, x, jnp.concatenate(parts, axis=0).T.astype(BF16))
        send(4 + k)
    for copy in copies:
        copy.wait()


def held_at(r_ref, array, x, j):
    pick = lambda part: r_ref[x // 2 * 4 + j, part, x % 2].astype(F32)
    if array < 2:
        return pick(2 * array) + pick(2 * array + 1)
    return pick(2 + array)


def collect_body(place, in_ref, q_ref, p_ref):
    for k, ref in enumerate((q_ref, p_ref)):
        chans = ref.shape[0]
        for x in range(ref.shape[1]):
            rows = [None] * len(place)
            for member, block in enumerate(place):
                rows[block] = in_ref[member, k, x]
            flat = jnp.concatenate(rows, axis=0).T
            for y in range(ref.shape[2]):
                ref[:, x, y, :] = flat[y * chans : (y + 1) * chans, :]


def weights_body(near, m_ref, out_ref, top_ref, fwd_ref):
    groups = near[1]
    chans = near[0] * m_ref.shape[1]
    per = chans // groups
    taps = 27
    at = lax.broadcasted_iota(jnp.int32, (chans, chans), 0)
    row = at % (2 * near[0]) // 2 * (chans // near[0]) + at // (2 * near[0]) * 2 + at % 2
    swap = (row == lax.broadcasted_iota(jnp.int32, (chans, chans), 1)).astype(BF16)
    turned = []
    for g in range(groups):
        m = jnp.concatenate([m_ref[a * groups + g] for a in range(near[0])], axis=0)
        m = jnp.dot(swap, m, preferred_element_type=F32)
        turned.append(m.T.astype(BF16))
    for f in range(2):
        for tap in range(taps):
            at = (f * taps + tap) * per
            for g in range(groups):
                fwd_ref[f, tap * chans + g * per : tap * chans + (g + 1) * per, :] = turned[g][
                    at : at + per, :
                ].astype(F32)
    zero = jnp.zeros((chans, chans), BF16)

    def store(w, a, row, u, block):
        row = row * chans
        if a < 2:
            col = (a * 2 + u) * chans
            out_ref[w, row : row + chans, col : col + chans] = block
            return
        for pair in range(2):
            at, col = row + pair * 6 * chans, (pair * 2 + u) * chans
            top_ref[w, at : at + chans, col : col + chans] = block

    def place(w, tap, block):
        a, b, c = tap // 9, tap // 3 % 3, tap % 3
        for u in range(2):
            t = b + u
            store(w, a, (t // 2 * 3 + c) * 2 + t % 2, u, block)

    for w in range(4):
        top_ref[w, 0 : 6 * chans, 2 * chans :] = jnp.zeros((6 * chans, 2 * chans), BF16)
        top_ref[w, 12 * chans :, 0 : 2 * chans] = jnp.zeros((6 * chans, 2 * chans), BF16)
        for c in range(3):
            for a in range(3):
                for t, u in ((3, 0), (0, 1)):
                    store(w, a, (t // 2 * 3 + c) * 2 + t % 2, u, zero)
    for f in range(2):
        for tap in range(0, taps, 2):
            n = min(2, taps - tap)
            pair = fwd_ref[f, tap * chans : (tap + n) * chans, :]
            adj = pair.T
            for i in range(n):
                part = slice(i * chans, (i + 1) * chans)
                place(f, tap + i, pair[part].astype(BF16))
                place(f + 2, taps - 1 - tap - i, adj[:, part].astype(BF16))


def strips(r):
    high = r.astype(BF16).astype(F32)
    low = r - high
    upper = lax.broadcasted_iota(jnp.int32, (8, 128), 0) < HALO
    first = jnp.where(upper, high[:8], pltpu.roll(low[:8], HALO, 0))
    last = jnp.where(upper, pltpu.roll(high[-8:], HALO, 0), low[-8:])
    return first.astype(BF16), last.astype(BF16)


def ahead(coef, turns, q, p, n):
    decay, kick, half = coef
    c = turns * half * half * (1.0 + decay)
    return (1.0 - c) * q + half * (1.0 + decay) * p + half * kick * n, c


def prepare_body(coef, r_ref, block_ref, rl_ref, rh_ref):
    for x in range(XB):
        for j in range(4):
            q, p, n = (held_at(r_ref, k, x, j) for k in range(3))
            block_ref[x, j] = r_ref[x // 2 * 4 + j, 0, x % 2]
            rl_ref[x, j], rh_ref[x, j] = strips(ahead(coef, 1, q, p, n)[0])


def gradient_body(kind, wide, coef, *refs):
    decay, kick, half = coef
    it = iter(refs)
    r_ref = next(it)
    if kind == "first":
        q_of = lambda x, j: held_at(r_ref, 0, x, j)
        p_of = lambda x, j: held_at(r_ref, 1, x, j)
    else:
        q_ref, p_ref = next(it), next(it)
        q_of = lambda x, j: q_ref[x, j]
        p_of = lambda x, j: p_ref[x, j]
    step_at = {"first": 0}.get(kind, kind)
    noise_of = lambda x, j, k: held_at(r_ref, 2 + k, x, j)
    if wide:
        xl_ref, xh_ref, zl_ref, zh_ref, w_ref, w2_ref, bias_ref = (next(it) for _ in range(7))
    else:
        xl_ref, xh_ref, own_ref, w_ref, w2_ref, bias_ref = (next(it) for _ in range(6))
    if kind == "last":
        out_ref = next(it)
    else:
        qo_ref, po_ref, qb_ref = (next(it) for _ in range(3))
        if not wide:
            rl_ref, rh_ref = next(it), next(it)
    buf, rows_a, rows_b, act = (next(it) for _ in range(4))

    pad = 2 * HALO if wide else HALO
    pitch = ZB + 2 * pad
    x_all = XB + 2 * HALO
    lo, hi, end = 8 + pad, 8 + pad + ZB, 8 + pitch
    edge = jnp.zeros((x_all, 4, 8, 128), F32)
    buf[:, :, 0:8, :] = edge
    buf[:, :, end : end + 8, :] = edge
    if wide:
        buf[0:HALO, :, lo:hi, :] = xl_ref[...].astype(F32)
        buf[HALO + XB :, :, lo:hi, :] = xh_ref[...].astype(F32)
        for x in range(XB):
            for j in range(4):
                buf[HALO + x, j, lo:hi, :] = q_of(x, j)
        buf[:, :, 8:lo, :] = zl_ref[0:x_all].astype(F32)
        buf[:, :, hi:end, :] = zh_ref[0:x_all].astype(F32)
    else:
        buf[0:HALO, :, 8:end, :] = xl_ref[...].astype(F32)
        buf[HALO : HALO + XB, :, 8:end, :] = own_ref[...].astype(F32)
        buf[HALO + XB :, :, 8:end, :] = xh_ref[...].astype(F32)

    def build(j, x_in, rows):
        n = x_in * pitch
        for c in range(3):
            v = buf[0:x_in, j, 7 + c : 7 + c + pitch, :].reshape(n, 128).astype(BF16)
            rows[0:n, (j * 3 + c) * 128 : (j * 3 + c + 1) * 128] = v
            if j == 0:
                rows[0:n, (12 + c) * 128 : (13 + c) * 128] = v

    def conv(x_in, w, use, rows, then=None):
        n = x_in * pitch
        x_out = x_in - 2
        m = x_out * pitch
        for p in range(4):
            cols = slice(384 * p, 384 * p + 768)
            t = jnp.dot(rows[0 : n - pitch, cols], w_ref[w], preferred_element_type=F32)
            if p % 2 == 0:
                cols = slice(384 * p, 384 * p + 1152)
                top = jnp.dot(rows[2 * pitch : n, cols], w2_ref[w], preferred_element_type=F32)
            o = t[0:m, 0:128] + t[pitch:, 128:256] + top[:, p % 2 * 128 : p % 2 * 128 + 128]
            use(p, o.reshape(x_out, pitch, 128))
            if then is not None:
                build(p, x_out, then)

    def hidden(p, h):
        t = jnp.tanh(h + bias_ref[...])
        act[:, p] = 1.0 - t * t
        buf[0 : XB + 6, p, 8:end, :] = t

    def second(p, h):
        buf[0 : XB + 4, p, 8:end, :] = h

    def back(p, g):
        buf[0 : XB + 2, p, 8:end, :] = g * act[2 : XB + 4, (p + 1) % 4]

    def final(p, g):
        buf[0:XB, p, 8:end, :] = g
        j = (p + 2) % 4
        for x in range(XB):
            q = q_of(x, j)
            force = buf[x, p, lo:hi, :] + q
            mom = p_of(x, j) - half * force
            if kind == "last":
                out_ref[x // 2, j, 0, x % 2] = q
                out_ref[x // 2, j, 1, x % 2] = mom
                continue
            if kind != "first":
                mom = mom - half * force
            q = q + half * mom
            mom = decay * mom + kick * noise_of(x, j, step_at)
            q = q + half * mom
            qo_ref[x, j] = q
            po_ref[x, j] = mom
            if not wide:
                qb_ref[x, j] = q.astype(BF16)
                r, _ = ahead(coef, 2, q, mom, noise_of(x, j, step_at + 1))
                rl_ref[x, j], rh_ref[x, j] = strips(r)
                continue
            c = (1 if kind == "first" else 2) * half * half * (1.0 + decay)
            below, above = slice(lo - HALO, lo), slice(hi, hi + HALO)
            for ref, at in ((zl_ref, below), (zh_ref, above)):
                r = ref[x_all + x, j].astype(F32)
                r = r + pltpu.roll(r, HALO, 0)
                buf[x, p, at, :] = r[:HALO] - c * buf[x, p, at, :]
            buf[x, p, lo:hi, :] = q
            qb_ref[x, j] = buf[x, p, lo - HALO : hi + HALO, :].astype(BF16)

    for j in range(4):
        build(j, XB + 8, rows_a)
    conv(XB + 8, 0, hidden, rows_a, rows_b)
    conv(XB + 6, 1, second, rows_b, rows_a)
    conv(XB + 4, 3, back, rows_a, rows_b)
    conv(XB + 2, 2, final, rows_b)


def solution(mesh):
    gy, gz = mesh.shape["gy"], mesh.shape["gz"]
    gs = XB // 2
    gX = mesh.shape["gx"] // gs
    fine = Mesh(
        mesh.devices.reshape(mesh.shape["grp"], gX, gs, gy, gz), ("grp", "gX", "gs", "gy", "gz")
    )
    walk = cycle(gs, gy)
    place = [walk.index((a, b)) for a in range(gs) for b in range(gy)]
    ring = [(a * gy + b) * gz + c for c in range(gz) for a, b in walk]

    def x_shift(d):
        return [(i, (i + d) % gX) for i in range(gX)]

    def z_shift(d):
        n = len(ring)
        return [(ring[i], ring[(i + d) % n]) for i in range(n)]

    decay = math.exp(-0.25)
    kick = math.sqrt(1.0 - decay * decay)

    def along_x(block):
        xl = lax.ppermute(block, "gX", x_shift(1))
        xh = lax.ppermute(block, "gX", x_shift(-1))
        return xl, xh

    def swapped_along_x(block):
        def swaps(first):
            pairs = [(i, (i + 1) % gX) for i in range(0 if first else 1, gX, 2)]
            return [pair for i, j in pairs for pair in ((i, j), (j, i))]

        one = lax.ppermute(block, "gX", swaps(True))
        two = lax.ppermute(block, "gX", swaps(False))
        even = lax.axis_index("gX") % 2 == 0
        return jnp.where(even, two, one), jnp.where(even, one, two)

    def along_both(block, rl, rh):
        xl, xh = along_x(block)
        whole = jnp.concatenate([xl, block, xh], axis=0)
        up = jnp.concatenate([whole[:, :, ZB - 2 * HALO :], rh], axis=0)
        down = jnp.concatenate([whole[:, :, : 2 * HALO], rl], axis=0)
        zl = lax.ppermute(up, ("gs", "gy", "gz"), z_shift(1))
        zh = lax.ppermute(down, ("gs", "gy", "gz"), z_shift(-1))
        return xl, xh, zl, zh

    def body(position, momentum, noise, filter_in, filter_out, bias):
        chans = position.shape[0]
        steps = noise.shape[0]
        members = gs * gy

        own = [f.reshape(*f.shape[:2], 27).transpose(0, 2, 1) for f in (filter_in, filter_out)]
        own = jnp.concatenate([f.reshape(f.shape[0], -1) for f in own], axis=1)
        own = jnp.pad(own, ((0, 0), (0, -own.shape[1] % 128)))
        far = lax.all_to_all(
            jnp.broadcast_to(own, (gX, *own.shape)), "gX", 0, 0, tiled=True
        )
        far = far.reshape(-1, far.shape[-1])
        near = lax.all_to_all(
            jnp.broadcast_to(far, (members, *far.shape)), ("gs", "gy"), 0, 0, tiled=True
        )
        weights = kernel_call(
            functools.partial(weights_body, (gs, gy)),
            [
                jax.ShapeDtypeStruct((4, 12 * chans, 4 * chans), BF16),
                jax.ShapeDtypeStruct((4, 18 * chans, 4 * chans), BF16),
            ],
            (near,),
            [VMEM((2, 27 * chans, chans), F32)],
        )
        bias_row = jnp.concatenate([bias, bias])[None, :]

        (spread,) = kernel_call(
            functools.partial(spread_body, place),
            [jax.ShapeDtypeStruct((members, 4 + steps, 2, ZB, 128), BF16)],
            (position, momentum, noise),
            [
                VMEM((members, 4 + steps, 2, ZB, 128), BF16),
                pltpu.SemaphoreType.DMA((4 + steps,)),
            ],
            hbm_in=True,
            hbm_out=True,
            out_space=pl.ANY,
        )
        held = lax.all_to_all(spread, ("gs", "gy"), 0, 0, tiled=True)

        coef = (decay, kick, 0.5 * STEP)
        tall = (XB, gy, ZB, 128)
        state32 = jax.ShapeDtypeStruct(tall, F32)
        block16 = jax.ShapeDtypeStruct(tall, BF16)
        grown16 = jax.ShapeDtypeStruct((XB, gy, ZB + 2 * HALO, 128), BF16)
        strip16 = jax.ShapeDtypeStruct((XB, gy, 2 * HALO, 128), BF16)
        block, *ends = kernel_call(
            functools.partial(prepare_body, coef), [block16, strip16, strip16], (held,)
        )
        state = ()
        for k in range(steps + 1):
            kind = "first" if k == 0 else "last" if k == steps else k
            wide = k % 2 == 0
            if wide:
                edges = along_both(block, *ends)
            else:
                swap = swapped_along_x if kind == "last" else along_x
                edges = (*swap(block), block)
            outs = [state32, state32, grown16] if wide else [state32, state32, block16, strip16, strip16]
            if kind == "last":
                outs = [jax.ShapeDtypeStruct((gs, gy, 2, 2, ZB, 128), F32)]
            pitch = ZB + (4 if wide else 2) * HALO
            res = kernel_call(
                functools.partial(gradient_body, kind, wide, coef),
                outs,
                (held, *state, *edges, *weights, bias_row),
                (
                    VMEM((XB + 8, gy, pitch + 16, 128), F32),
                    VMEM(((XB + 8) * pitch, 15 * 128), BF16),
                    VMEM(((XB + 6) * pitch, 15 * 128), BF16),
                    VMEM((XB + 6, gy, pitch, 128), F32),
                ),
            )
            if kind != "last":
                state, block, ends = tuple(res[:2]), res[2], res[3:]
        back = lax.all_to_all(
            res[0].reshape(members, 2, 2, ZB, 128), ("gs", "gy"), 0, 0, tiled=True
        )
        out = jax.ShapeDtypeStruct(position.shape, F32)
        return tuple(
            kernel_call(functools.partial(collect_body, place), [out, out], (back,), hbm_out=True)
        )

    where = ("grp", "gX", "gs")
    lattice = P(None, where, "gy", "gz")
    filters = P(("gX", "gs"), "gy", None, None, None)
    return jax.shard_map(
        body,
        mesh=fine,
        in_specs=(lattice, lattice, P(None, None, where, "gy", "gz"), filters, filters, P()),
        out_specs=(lattice, lattice),
        check_vma=False,
    )
```
